512 devices in a mesh: gx: 32 (over x, z), gy: 2 (over y_hi), gz: 8 (over y_lo, core).
Axes of the slice: x: 4, y: 8 (y_hi: 2, y_lo: 4; y = y_hi * 4 + y_lo), z: 8, core: 2. Of those that a mesh axis runs over, the one named last changes fastest.
Arguments:
- coeffs: bfloat16 [16, 1024, 160], P('gz', ('gx', 'gy')), may hold values from -6 to 6
- translations: bfloat16 [16384, 160, 160], P(('gx', 'gz'), 'gy'), may hold values from -0.25 to 0.25
- tmatrix: bfloat16 [1024, 160, 160], P('gx', 'gy'), may hold values from -0.5 to 0.5
- pair_target: int32 [16384], P('gx'), may hold values from 0 to 31
- pair_source: int32 [16384], P('gx'), may hold values from 0 to 1023, as said below
- pair_count: int32 [32], P('gx'), may hold values from 256 to 512, as said below
Outputs:
- result: bfloat16 [16, 1024, 160], P('gz', ('gx', 'gy'))
The draws below stay inside these ranges and needn't reach their ends.
Inputs may be any that keep to these rules, and one draw needn't show every extreme that they name: `pair_count`: some gx group has all 512 slots live in every draw. The source sphere of a slot of group g lies in group g - 1, g or g + 1 modulo 32, that is pair_source[p] // 32 is one of these.
All inputs are finite; a program needn't handle non-finite values.
Results may differ from the reference program's by a relative error of at most 0.009.
Values may be sent and summed in bfloat16 or wider, within the bound.
A program may use at most 64 MiB of HBM per device.

```python
import jax
import jax.numpy as jnp
from jax import lax

L = 160
R = 16
SPH_X = 32
GROUPS = 32
SPHERES = 1024
PAIR_GRP = 512
PAIRS = 16384


def draw_pair_count(key, part):
    counts = jax.random.randint(key, (GROUPS,), PAIR_GRP // 2, PAIR_GRP + 1)
    fullest = jax.random.randint(jax.random.fold_in(key, 7), (), 0, GROUPS)
    return jnp.where(jnp.arange(GROUPS) == fullest, PAIR_GRP, counts).astype(jnp.int32)


def draw_pair_source(key, part):
    owner = (jnp.arange(PAIRS, dtype=jnp.int32) // PAIR_GRP).astype(jnp.int32)
    offset = jax.random.randint(jax.random.fold_in(key, 11), (PAIRS,), -1, 2)
    within = jax.random.randint(jax.random.fold_in(key, 13), (PAIRS,), 0, SPH_X)
    group = (owner + offset + GROUPS) % GROUPS
    return (group * SPH_X + within).astype(jnp.int32)


def place_ends(drawn, rng, smallest, top_value):
    place = [jax.random.randint(jax.random.fold_in(rng, axis), (), 0, length) for axis, length in enumerate(drawn.shape)]
    longest = drawn.shape.index(max(drawn.shape))
    next_to = place[:longest] + [(place[longest] + 1) % drawn.shape[longest]] + place[longest + 1:]
    return drawn.at[tuple(place)].set(smallest).at[tuple(next_to)].set(top_value)


def block_scale(stream_key, shape, split, least, largest):
    level = 1.0
    for dim, parts in split:
        steps = jax.random.uniform(jax.random.fold_in(jax.random.fold_in(stream_key, 6), dim), (parts,), jnp.float32, least / len(split), largest / len(split))
        level = level * jnp.repeat(jnp.exp(steps), shape[dim] // parts).reshape((-1,) + (1,) * (len(shape) - 1 - dim))
    return level


def gaussian(key, extent, deviation, most, pieces=(), held_as=jnp.bfloat16):
    drawn = deviation * jax.random.normal(key, extent, jnp.float32)
    if pieces:
        drawn = drawn * block_scale(key, extent, pieces, -0.22, 0.18)
    return jnp.clip(drawn, -most, most).astype(held_as)


def setup_inputs(seed: int = 0) -> dict:
    arg_keys = jax.random.split(jax.random.key(seed), 7)
    return {
        "coeffs": gaussian(arg_keys[0], (R, SPHERES, L), 1.0, 6.0, ((0, 8), (1, 64))),
        "translations": gaussian(arg_keys[1], (PAIRS, L, L), (4 * L) ** -0.5, 0.25, ((0, 256), (1, 2))),
        "tmatrix": gaussian(arg_keys[2], (SPHERES, L, L), L ** -0.5, 0.5, ((0, 32), (1, 2))),
        "pair_target": place_ends(jax.random.randint(arg_keys[3], (PAIRS,), 0, SPH_X), jax.random.fold_in(arg_keys[3], 1), 0, SPH_X - 1).astype(jnp.int32),
        "pair_source": draw_pair_source(jax.random.fold_in(arg_keys[6], 71), 0),
        "pair_count": draw_pair_count(jax.random.fold_in(arg_keys[6], 71), 0),
    }


def one_group(coeffs, group_data):
    blocks, target, source, live_count, tmat, own_rows = group_data
    picked = jnp.take(coeffs, source, axis=1).astype(jnp.float32)
    contrib = jnp.einsum('pkl,rpl->rpk', blocks.astype(jnp.float32), picked)
    living = jnp.arange(PAIR_GRP).astype(jnp.int32) < live_count
    spheres_here = jnp.arange(SPH_X).astype(jnp.int32)
    select = ((target[None, :] == spheres_here[:, None]) & living[None, :]).astype(jnp.float32)
    near_field = jnp.einsum('sp,rpk->rsk', select, contrib).astype(jnp.bfloat16)
    scattered = jnp.einsum('rsc,sci->rsi', near_field.astype(jnp.float32), tmat.astype(jnp.float32))
    return (own_rows.astype(jnp.float32) - scattered).astype(jnp.bfloat16)


def reference(coeffs, translations, tmatrix, pair_target, pair_source, pair_count):
    blocks = translations.reshape(GROUPS, PAIR_GRP, L, L)
    targets = pair_target.reshape(GROUPS, PAIR_GRP)
    sources = pair_source.reshape(GROUPS, PAIR_GRP)
    tmats = tmatrix.reshape(GROUPS, SPH_X, L, L)
    own_rows = coeffs.reshape(R, GROUPS, SPH_X, L).transpose(1, 0, 2, 3)
    outputs = lax.map(lambda item: one_group(coeffs, item), (blocks, targets, sources, pair_count, tmats, own_rows))
    return outputs.transpose(1, 0, 2, 3).reshape(R, SPHERES, L)
```

```python
import functools

import jax
import jax.numpy as jnp
from jax import lax
from jax.experimental import pallas as pl
from jax.experimental.pallas import tpu as pltpu
from jax.sharding import PartitionSpec as P

MESH = pl.DeviceIdType.MESH
F32 = jnp.float32
BF16 = jnp.bfloat16
NT = (((1,), (1,)), ((), ()))
RING = 8
NEAR_FIRST = (1, 7, 2, 6, 3, 5, 4)
FAR_FIRST = (4, 3, 5, 2, 6, 1, 7)


def packed_rows(rows):
    tails = [rows[8 * j : 8 * j + 8, 128:160] for j in range(4)]
    tail = jnp.concatenate(tails, axis=1)
    return jnp.concatenate([rows[:, :128], tail, jnp.zeros_like(tail)], axis=0)


def tail_rows(tail):
    return jnp.concatenate([tail[:, 32 * j : 32 * j + 32] for j in range(4)], axis=0)


def kernel(
    groups, count, target, source, coeffs_hbm, trans_hbm, tmat_hbm, out,
    coeffs, trans, tmat, win, tails, pick, place, picked, contrib, near, scat, parts, sums,
    local_sem, send_y, send_z, recv, pair_send, pair_recv, send_out, recv_out,
):
    gx, gy, gz = lax.axis_index("gx"), lax.axis_index("gy"), lax.axis_index("gz")
    quarter, core = gz // 2, gz % 2
    here = gy * 4 + quarter
    half = trans_hbm.shape[0]
    pairs = 2 * half

    def at(y):
        return {"gx": gx, "gy": y // 4, "gz": (y % 4) * 2 + core}

    up = {"gx": (gx + 1) % groups, "gy": gy, "gz": gz}
    down = {"gx": (gx + groups - 1) % groups, "gy": gy, "gz": gz}
    sibling = {"gx": gx, "gy": gy, "gz": quarter * 2 + 1 - core}

    load_c = pltpu.make_async_copy(coeffs_hbm, coeffs, local_sem.at[0])
    load_t = pltpu.make_async_copy(trans_hbm, trans.at[pl.ds(core * half, half)], local_sem.at[1])
    load_m = pltpu.make_async_copy(tmat_hbm, tmat, local_sem.at[2])
    load_c.start()
    load_t.start()
    load_m.start()

    barrier = pltpu.get_barrier_semaphore()
    for d in FAR_FIRST:
        pl.semaphore_signal(barrier, inc=1, device_id=at((here + d) % RING), device_id_type=MESH)
    for peer in (up, down, sibling):
        pl.semaphore_signal(barrier, inc=1, device_id=peer, device_id_type=MESH)

    load_c.wait()
    own = coeffs[...].astype(F32).reshape(32, 160)
    win[RING + here] = packed_rows(own).astype(BF16)

    lane = lax.broadcasted_iota(jnp.int32, (8, 128), 1)
    sub = lax.broadcasted_iota(jnp.int32, (8, 128), 0)
    diagonal = lane - 16 * sub

    def build_pick(j, carry):
        codes = []
        for u in range(2):
            s = source[quarter * pairs + 2 * j + u]
            relative = (s // 32 - gx + 1 + groups) % groups
            codes.append((relative * 2 + (s % 32) // 16) * 1024 + s % 16)
        for t in range(6):
            hot = [jnp.where(diagonal == c - 1024 * t, 1.0, 0.0) for c in codes]
            pick[pl.ds(pl.multiple_of(16 * j, 16), 16), 128 * t : 128 * t + 128] = jnp.concatenate(hot, axis=0).astype(BF16)
        return carry

    lax.fori_loop(0, pairs // 2, build_pick, 0)

    def build_place(q, carry):
        v = jnp.full((8, 128), -1, jnp.int32)
        for i in range(16):
            slot = quarter * pairs + q * 16 + i
            t = jnp.where(slot < count[0], target[slot], -1)
            v = jnp.where((lane // 8 == i) & (lane % 8 == sub), t, v)
        for s in range(16):
            hot = [jnp.where(v == 2 * s + u, 1.0, 0.0) for u in range(2)]
            place[16 * s : 16 * s + 16, pl.ds(pl.multiple_of(128 * q, 128), 128)] = jnp.concatenate(hot, axis=0).astype(BF16)
        return carry

    lax.fori_loop(0, pairs // 16, build_place, 0)

    load_t.wait()
    pl.semaphore_wait(barrier, 10)

    def remote(src, dst, s, r, peer):
        return pltpu.make_async_remote_copy(
            src_ref=src, dst_ref=dst, send_sem=s, recv_sem=r, device_id=peer, device_id_type=MESH
        )

    sends = []

    def start(copy):
        copy.start()
        sends.append(copy)

    def forward(y):
        block = win.at[RING + y]
        start(remote(block, win.at[y], send_z.at[y], recv.at[y], up))
        start(remote(block, win.at[2 * RING + y], send_z.at[RING + y], recv.at[2 * RING + y], down))

    def unpack(slot):
        tail = tail_rows(win[slot, 32:48, :].astype(F32)[0:8])
        tails[slot] = tail.astype(BF16)

    def arrive(slot):
        remote(win.at[slot], win.at[slot], send_y.at[0], recv.at[slot], sibling).wait_recv()

    for d in FAR_FIRST:
        start(remote(win.at[RING + here], win.at[RING + here], send_y.at[d], recv.at[RING + here], at((here + d) % RING)))
    forward(here)
    mine = trans.at[pl.ds(core * half, half)]
    start(remote(mine, mine, pair_send, pair_recv, sibling))
    unpack(RING + here)
    for d in NEAR_FIRST:
        y = (here + d) % RING
        arrive(RING + y)
        forward(y)
        unpack(RING + y)

    def group_rows(g):
        block = win[8 * g : 8 * g + 8, 0:32, :].reshape(256, 128)
        return jnp.concatenate([block, tails[8 * g : 8 * g + 8].reshape(256, 32)], axis=1)

    def pick_group(g, q):
        rows = pick[pl.ds(pl.multiple_of(128 * q, 128), 128), 256 * g : 256 * g + 256]
        return jnp.dot(rows, group_rows(g), preferred_element_type=F32).astype(BF16)

    def pick_own(q, carry):
        picked[q] = pick_group(1, q)
        return carry

    lax.fori_loop(0, 8, pick_own, 0)

    for d in (0,) + NEAR_FIRST:
        y = (here + d) % RING
        for slot in (y, 2 * RING + y):
            arrive(slot)
            unpack(slot)
    remote(mine, trans.at[pl.ds((1 - core) * half, half)], pair_send, pair_recv, sibling).wait_recv()

    chosen = lax.broadcasted_iota(jnp.int32, (16, 80, 128), 2) // 8 == lax.broadcasted_iota(jnp.int32, (16, 80, 128), 0)

    def translate(q, carry):
        rows = picked[q] + pick_group(0, q) + pick_group(2, q)
        blocks = trans[pl.ds(16 * q, 16)].reshape(1280, 160)
        every = lax.dot_general(blocks, rows, NT, preferred_element_type=F32).reshape(16, 80, 128)
        contrib[:, pl.ds(pl.multiple_of(128 * q, 128), 128)] = jnp.where(chosen, every, 0.0).sum(axis=0).astype(BF16)
        return carry

    lax.fori_loop(0, pairs // 16, translate, 0)

    near[...] = lax.dot_general(place[...], contrib[...], NT, preferred_element_type=F32).astype(BF16)
    load_m.wait()

    def scatter(j, carry):
        rows = near[pl.ds(pl.multiple_of(16 * j, 16), 16), :]
        for u in range(2):
            both = jnp.dot(rows, tmat[2 * j + u], preferred_element_type=F32)
            scat[2 * j + u] = both[8 * u : 8 * u + 8]
        return carry

    lax.fori_loop(0, 16, scatter, 0)

    for y in range(RING):
        h, r = y // 4, 2 * (y % 4)
        rows = jnp.concatenate([scat[16 * h : 16 * h + 16, r + u, :] for u in range(2)], axis=0)
        parts[y] = packed_rows(rows).astype(BF16)
    for d in FAR_FIRST:
        y = (here + d) % RING
        start(remote(parts.at[y], sums.at[here], send_out.at[d], recv_out.at[here], at(y)))
    total = parts[here].astype(F32)
    for d in NEAR_FIRST:
        y = (here + d) % RING
        remote(parts.at[y], sums.at[y], send_out.at[d], recv_out.at[y], sibling).wait_recv()
        total = total + sums[y].astype(F32)
    whole = jnp.concatenate([total[0:32], tail_rows(total[32:40])], axis=1)
    out[...] = (coeffs[...].astype(F32) - whole.reshape(2, 16, 160)).astype(BF16)
    for copy in sends:
        copy.wait_send()


def solution(mesh):
    groups = mesh.shape["gx"]

    def step(coeffs, translations, tmatrix, pair_target, pair_source, pair_count):
        half = translations.shape[0]
        smem = pl.BlockSpec(memory_space=pltpu.SMEM)
        hbm = pl.BlockSpec(memory_space=pl.ANY)
        return pl.pallas_call(
            functools.partial(kernel, groups),
            out_shape=jax.ShapeDtypeStruct(coeffs.shape, BF16),
            in_specs=[smem, smem, smem, hbm, hbm, hbm],
            out_specs=pl.BlockSpec(memory_space=pltpu.VMEM),
            scratch_shapes=[
                pltpu.VMEM(coeffs.shape, BF16),
                pltpu.VMEM((2 * half, 80, 160), BF16),
                pltpu.VMEM((32, 80, 160), BF16),
                pltpu.VMEM((24, 48, 128), BF16),
                pltpu.VMEM((24, 32, 32), BF16),
                pltpu.VMEM((1024, 768), BF16),
                pltpu.VMEM((256, 1024), BF16),
                pltpu.VMEM((8, 128, 160), BF16),
                pltpu.VMEM((80, 1024), BF16),
                pltpu.VMEM((256, 80), BF16),
                pltpu.VMEM((32, 8, 160), F32),
                pltpu.VMEM((8, 48, 128), BF16),
                pltpu.VMEM((8, 48, 128), BF16),
                pltpu.SemaphoreType.DMA((3,)),
                pltpu.SemaphoreType.DMA((8,)),
                pltpu.SemaphoreType.DMA((16,)),
                pltpu.SemaphoreType.DMA((24,)),
                pltpu.SemaphoreType.DMA,
                pltpu.SemaphoreType.DMA,
                pltpu.SemaphoreType.DMA((8,)),
                pltpu.SemaphoreType.DMA((8,)),
            ],
            compiler_params=pltpu.CompilerParams(
                collective_id=0, has_side_effects=True, vmem_limit_bytes=40 << 20
            ),
        )(pair_count, pair_target, pair_source, coeffs, translations, tmatrix)

    placed = (
        P("gz", ("gx", "gy"), None),
        P(("gx", "gz"), "gy", None),
        P("gx", "gy", None),
        P("gx"),
        P("gx"),
        P("gx"),
    )
    return jax.shard_map(
        step, mesh=mesh, in_specs=placed, out_specs=P("gz", ("gx", "gy"), None), check_vma=False
    )
```

```python
import functools

import jax
import jax.numpy as jnp
from jax import lax
from jax.experimental import pallas as pl
from jax.experimental.pallas import tpu as pltpu
from jax.sharding import PartitionSpec as P

MESH = pl.DeviceIdType.MESH
F32 = jnp.float32
BF16 = jnp.bfloat16
NT = (((1,), (1,)), ((), ()))
RING = 8
NEAR_FIRST = (1, 7, 2, 6, 3, 5, 4)
FAR_FIRST = (4, 3, 5, 2, 6, 1, 7)


def packed_rows(rows):
    tails = [rows[8 * j : 8 * j + 8, 128:160] for j in range(4)]
    tail = jnp.concatenate(tails, axis=1)
    return jnp.concatenate([rows[:, :128], tail, jnp.zeros_like(tail)], axis=0)


def tail_rows(tail):
    return jnp.concatenate([tail[:, 32 * j : 32 * j + 32] for j in range(4)], axis=0)


def kernel(
    groups, count_hbm, target_hbm, source_hbm, coeffs_hbm, trans_hbm, tmat_hbm, out,
    count, target, source, coeffs, trans, tmat, win, tails, pick, place, picked, contrib, near, scat, parts, sums,
    local_sem, send_y, send_z, recv, pair_send, pair_recv, send_out, recv_out,
):
    gx, gy, gz = lax.axis_index("gx"), lax.axis_index("gy"), lax.axis_index("gz")
    quarter, core = gz // 2, gz % 2
    here = gy * 4 + quarter
    half = trans_hbm.shape[0]
    pairs = 2 * half

    def at(y):
        return {"gx": gx, "gy": y // 4, "gz": (y % 4) * 2 + core}

    up = {"gx": (gx + 1) % groups, "gy": gy, "gz": gz}
    down = {"gx": (gx + groups - 1) % groups, "gy": gy, "gz": gz}
    sibling = {"gx": gx, "gy": gy, "gz": quarter * 2 + 1 - core}

    load_c = pltpu.make_async_copy(coeffs_hbm, coeffs, local_sem.at[0])
    load_t = pltpu.make_async_copy(trans_hbm, trans.at[pl.ds(core * half, half)], local_sem.at[1])
    load_m = pltpu.make_async_copy(tmat_hbm, tmat, local_sem.at[2])
    load_p = [
        pltpu.make_async_copy(count_hbm, count, local_sem.at[3]),
        pltpu.make_async_copy(target_hbm, target, local_sem.at[4]),
        pltpu.make_async_copy(source_hbm, source, local_sem.at[5]),
    ]
    load_c.start()
    for load in load_p:
        load.start()
    load_t.start()
    load_m.start()

    barrier = pltpu.get_barrier_semaphore()
    for d in FAR_FIRST:
        pl.semaphore_signal(barrier, inc=1, device_id=at((here + d) % RING), device_id_type=MESH)
    for peer in (up, down, sibling):
        pl.semaphore_signal(barrier, inc=1, device_id=peer, device_id_type=MESH)

    load_c.wait()
    own = coeffs[...].astype(F32).reshape(32, 160)
    win[RING + here] = packed_rows(own).astype(BF16)

    for load in load_p:
        load.wait()
    lane = lax.broadcasted_iota(jnp.int32, (8, 128), 1)
    sub = lax.broadcasted_iota(jnp.int32, (8, 128), 0)
    diagonal = lane - 16 * sub

    def build_pick(j, carry):
        codes = []
        for u in range(2):
            s = source[quarter * pairs + 2 * j + u]
            relative = (s // 32 - gx + 1 + groups) % groups
            codes.append((relative * 2 + (s % 32) // 16) * 1024 + s % 16)
        for t in range(6):
            hot = [jnp.where(diagonal == c - 1024 * t, 1.0, 0.0) for c in codes]
            pick[pl.ds(pl.multiple_of(16 * j, 16), 16), 128 * t : 128 * t + 128] = jnp.concatenate(hot, axis=0).astype(BF16)
        return carry

    lax.fori_loop(0, pairs // 2, build_pick, 0)

    def build_place(q, carry):
        v = jnp.full((8, 128), -1, jnp.int32)
        for i in range(16):
            slot = quarter * pairs + q * 16 + i
            t = jnp.where(slot < count[0], target[slot], -1)
            v = jnp.where((lane // 8 == i) & (lane % 8 == sub), t, v)
        for s in range(16):
            hot = [jnp.where(v == 2 * s + u, 1.0, 0.0) for u in range(2)]
            place[16 * s : 16 * s + 16, pl.ds(pl.multiple_of(128 * q, 128), 128)] = jnp.concatenate(hot, axis=0).astype(BF16)
        return carry

    lax.fori_loop(0, pairs // 16, build_place, 0)

    load_t.wait()
    pl.semaphore_wait(barrier, 10)

    def remote(src, dst, s, r, peer):
        return pltpu.make_async_remote_copy(
            src_ref=src, dst_ref=dst, send_sem=s, recv_sem=r, device_id=peer, device_id_type=MESH
        )

    sends = []

    def start(copy):
        copy.start()
        sends.append(copy)

    def forward(y):
        block = win.at[RING + y]
        start(remote(block, win.at[y], send_z.at[y], recv.at[y], up))
        start(remote(block, win.at[2 * RING + y], send_z.at[RING + y], recv.at[2 * RING + y], down))

    def unpack(slot):
        tail = tail_rows(win[slot, 32:48, :].astype(F32)[0:8])
        tails[slot] = tail.astype(BF16)

    def arrive(slot):
        remote(win.at[slot], win.at[slot], send_y.at[0], recv.at[slot], sibling).wait_recv()

    for d in FAR_FIRST:
        start(remote(win.at[RING + here], win.at[RING + here], send_y.at[d], recv.at[RING + here], at((here + d) % RING)))
    forward(here)
    mine = trans.at[pl.ds(core * half, half)]
    start(remote(mine, mine, pair_send, pair_recv, sibling))
    unpack(RING + here)
    for d in NEAR_FIRST:
        y = (here + d) % RING
        arrive(RING + y)
        forward(y)
        unpack(RING + y)

    def group_rows(g):
        block = win[8 * g : 8 * g + 8, 0:32, :].reshape(256, 128)
        return jnp.concatenate([block, tails[8 * g : 8 * g + 8].reshape(256, 32)], axis=1)

    def pick_group(g, q):
        rows = pick[pl.ds(pl.multiple_of(128 * q, 128), 128), 256 * g : 256 * g + 256]
        return jnp.dot(rows, group_rows(g), preferred_element_type=F32).astype(BF16)

    def pick_own(q, carry):
        picked[q] = pick_group(1, q)
        return carry

    lax.fori_loop(0, 8, pick_own, 0)

    for d in (0,) + NEAR_FIRST:
        y = (here + d) % RING
        for slot in (y, 2 * RING + y):
            arrive(slot)
            unpack(slot)
    remote(mine, trans.at[pl.ds((1 - core) * half, half)], pair_send, pair_recv, sibling).wait_recv()

    chosen = lax.broadcasted_iota(jnp.int32, (16, 80, 128), 2) // 8 == lax.broadcasted_iota(jnp.int32, (16, 80, 128), 0)

    def translate(q, carry):
        rows = picked[q] + pick_group(0, q) + pick_group(2, q)
        blocks = trans[pl.ds(16 * q, 16)].reshape(1280, 160)
        every = lax.dot_general(blocks, rows, NT, preferred_element_type=F32).reshape(16, 80, 128)
        contrib[:, pl.ds(pl.multiple_of(128 * q, 128), 128)] = jnp.where(chosen, every, 0.0).sum(axis=0).astype(BF16)
        return carry

    lax.fori_loop(0, pairs // 16, translate, 0)

    near[...] = lax.dot_general(place[...], contrib[...], NT, preferred_element_type=F32).astype(BF16)
    load_m.wait()

    def scatter(j, carry):
        rows = near[pl.ds(pl.multiple_of(16 * j, 16), 16), :]
        for u in range(2):
            both = jnp.dot(rows, tmat[2 * j + u], preferred_element_type=F32)
            scat[2 * j + u] = both[8 * u : 8 * u + 8]
        return carry

    lax.fori_loop(0, 16, scatter, 0)

    for y in range(RING):
        h, r = y // 4, 2 * (y % 4)
        rows = jnp.concatenate([scat[16 * h : 16 * h + 16, r + u, :] for u in range(2)], axis=0)
        parts[y] = packed_rows(rows).astype(BF16)
    for d in FAR_FIRST:
        y = (here + d) % RING
        start(remote(parts.at[y], sums.at[here], send_out.at[d], recv_out.at[here], at(y)))
    total = parts[here].astype(F32)
    for d in NEAR_FIRST:
        y = (here + d) % RING
        remote(parts.at[y], sums.at[y], send_out.at[d], recv_out.at[y], sibling).wait_recv()
        total = total + sums[y].astype(F32)
    whole = jnp.concatenate([total[0:32], tail_rows(total[32:40])], axis=1)
    out[...] = (coeffs[...].astype(F32) - whole.reshape(2, 16, 160)).astype(BF16)
    for copy in sends:
        copy.wait_send()


def solution(mesh):
    groups = mesh.shape["gx"]

    def step(coeffs, translations, tmatrix, pair_target, pair_source, pair_count):
        half = translations.shape[0]
        hbm = pl.BlockSpec(memory_space=pltpu.HBM)
        return pl.pallas_call(
            functools.partial(kernel, groups),
            out_shape=jax.ShapeDtypeStruct(coeffs.shape, BF16),
            in_specs=[hbm] * 6,
            out_specs=pl.BlockSpec(memory_space=pltpu.VMEM),
            scratch_shapes=[
                pltpu.SMEM(pair_count.shape, jnp.int32),
                pltpu.SMEM(pair_target.shape, jnp.int32),
                pltpu.SMEM(pair_source.shape, jnp.int32),
                pltpu.VMEM(coeffs.shape, BF16),
                pltpu.VMEM((2 * half, 80, 160), BF16),
                pltpu.VMEM((32, 80, 160), BF16),
                pltpu.VMEM((24, 48, 128), BF16),
                pltpu.VMEM((24, 32, 32), BF16),
                pltpu.VMEM((1024, 768), BF16),
                pltpu.VMEM((256, 1024), BF16),
                pltpu.VMEM((8, 128, 160), BF16),
                pltpu.VMEM((80, 1024), BF16),
                pltpu.VMEM((256, 80), BF16),
                pltpu.VMEM((32, 8, 160), F32),
                pltpu.VMEM((8, 48, 128), BF16),
                pltpu.VMEM((8, 48, 128), BF16),
                pltpu.SemaphoreType.DMA((6,)),
                pltpu.SemaphoreType.DMA((8,)),
                pltpu.SemaphoreType.DMA((16,)),
                pltpu.SemaphoreType.DMA((24,)),
                pltpu.SemaphoreType.DMA,
                pltpu.SemaphoreType.DMA,
                pltpu.SemaphoreType.DMA((8,)),
                pltpu.SemaphoreType.DMA((8,)),
            ],
            compiler_params=pltpu.CompilerParams(
                collective_id=0, has_side_effects=True, vmem_limit_bytes=67_043_328
            ),
        )(pair_count, pair_target, pair_source, coeffs, translations, tmatrix)

    placed = (
        P("gz", ("gx", "gy"), None),
        P(("gx", "gz"), "gy", None),
        P("gx", "gy", None),
        P("gx"),
        P("gx"),
        P("gx"),
    )
    return jax.shard_map(
        step, mesh=mesh, in_specs=placed, out_specs=P("gz", ("gx", "gy"), None), check_vma=False
    )
```

```python
import functools

import jax
import jax.numpy as jnp
from jax import lax
from jax.experimental import pallas as pl
from jax.experimental.pallas import tpu as pltpu
from jax.sharding import PartitionSpec as P

MESH = pl.DeviceIdType.MESH
F32 = jnp.float32
BF16 = jnp.bfloat16
NT = (((1,), (1,)), ((), ()))
RING = 8
NEAR_FIRST = (1, 7, 2, 6, 3, 5, 4)
FAR_FIRST = (4, 3, 5, 2, 6, 1, 7)


def packed_rows(rows):
    tails = [rows[8 * j : 8 * j + 8, 128:160] for j in range(4)]
    tail = jnp.concatenate(tails, axis=1)
    return jnp.concatenate([rows[:, :128], tail, jnp.zeros_like(tail)], axis=0)


def tail_rows(tail):
    return jnp.concatenate([tail[:, 32 * j : 32 * j + 32] for j in range(4)], axis=0)


def kernel(
    groups, count, target_hbm, source_hbm, coeffs_hbm, trans_hbm, tmat_hbm, out,
    target, source, coeffs, trans, tmat, win, tails, pick, place, picked, contrib, near, scat, parts, sums,
    local_sem, send_y, send_z, recv, pair_send, pair_recv, send_out, recv_out,
):
    load_c = pltpu.make_async_copy(coeffs_hbm, coeffs, local_sem.at[0])
    load_c.start()

    gx, gy, gz = lax.axis_index("gx"), lax.axis_index("gy"), lax.axis_index("gz")
    quarter, core = gz // 2, gz % 2
    here = gy * 4 + quarter
    half = trans_hbm.shape[0]
    pairs = 2 * half

    def at(y):
        return {"gx": gx, "gy": y // 4, "gz": (y % 4) * 2 + core}

    up = {"gx": (gx + 1) % groups, "gy": gy, "gz": gz}
    down = {"gx": (gx + groups - 1) % groups, "gy": gy, "gz": gz}
    sibling = {"gx": gx, "gy": gy, "gz": quarter * 2 + 1 - core}
    ring = [(here + d) % RING for d in range(RING)]

    barrier = pltpu.get_barrier_semaphore()
    for d in FAR_FIRST:
        pl.semaphore_signal(barrier, inc=1, device_id=at(ring[d]), device_id_type=MESH)
    for peer in (up, down, sibling):
        pl.semaphore_signal(barrier, inc=1, device_id=peer, device_id_type=MESH)

    load_p = [
        pltpu.make_async_copy(target_hbm, target, local_sem.at[3]),
        pltpu.make_async_copy(source_hbm, source, local_sem.at[4]),
    ]
    load_t = pltpu.make_async_copy(trans_hbm, trans.at[pl.ds(core * half, half)], local_sem.at[1])
    load_m = pltpu.make_async_copy(tmat_hbm, tmat, local_sem.at[2])
    for load in load_p:
        load.start()
    load_t.start()
    load_m.start()

    load_c.wait()
    own = coeffs[...].astype(F32).reshape(32, 160)
    win[RING + here] = packed_rows(own).astype(BF16)

    pl.semaphore_wait(barrier, 10)

    def remote(src, dst, s, r, peer):
        return pltpu.make_async_remote_copy(
            src_ref=src, dst_ref=dst, send_sem=s, recv_sem=r, device_id=peer, device_id_type=MESH
        )

    sends = []

    def start(copy):
        copy.start()
        sends.append(copy)

    def forward(y):
        block = win.at[RING + y]
        start(remote(block, win.at[y], send_z.at[y], recv.at[y], up))
        start(remote(block, win.at[2 * RING + y], send_z.at[RING + y], recv.at[2 * RING + y], down))

    def unpack(slot):
        tail = tail_rows(win[slot, 32:48, :].astype(F32)[0:8])
        tails[slot] = tail.astype(BF16)

    def arrive(slot):
        remote(win.at[slot], win.at[slot], send_y.at[0], recv.at[slot], sibling).wait_recv()

    for d in FAR_FIRST:
        start(remote(win.at[RING + here], win.at[RING + here], send_y.at[d], recv.at[RING + here], at(ring[d])))
    forward(here)
    load_t.wait()
    mine = trans.at[pl.ds(core * half, half)]
    start(remote(mine, mine, pair_send, pair_recv, sibling))

    for load in load_p:
        load.wait()
    lane = lax.broadcasted_iota(jnp.int32, (8, 128), 1)
    sub = lax.broadcasted_iota(jnp.int32, (8, 128), 0)
    diagonal = lane - 16 * sub

    def build_pick(j, carry):
        for v in range(4):
            codes = []
            for u in range(2):
                s = source[quarter * pairs + 8 * j + 2 * v + u]
                relative = (s // 32 - gx + 1 + groups) % groups
                codes.append((relative * 2 + (s % 32) // 16) * 1024 + s % 16)
            rows = pl.ds(pl.multiple_of(64 * j + 16 * v, 16), 16)
            for t in range(6):
                hot = [jnp.where(diagonal == c - 1024 * t, 1.0, 0.0) for c in codes]
                pick[rows, 128 * t : 128 * t + 128] = jnp.concatenate(hot, axis=0).astype(BF16)
        return carry

    lax.fori_loop(0, pairs // 8, build_pick, 0)

    for d in NEAR_FIRST:
        arrive(RING + ring[d])
        forward(ring[d])

    def build_place(q, carry):
        v = jnp.full((8, 128), -1, jnp.int32)
        for i in range(16):
            slot = quarter * pairs + q * 16 + i
            t = jnp.where(slot < count[0], target[slot], -1)
            v = jnp.where((lane // 8 == i) & (lane % 8 == sub), t, v)
        for s in range(16):
            hot = [jnp.where(v == 2 * s + u, 1.0, 0.0) for u in range(2)]
            place[16 * s : 16 * s + 16, pl.ds(pl.multiple_of(128 * q, 128), 128)] = jnp.concatenate(hot, axis=0).astype(BF16)
        return carry

    lax.fori_loop(0, pairs // 16, build_place, 0)

    def group_rows(g):
        for y in range(RING):
            unpack(RING * g + y)
        block = win[8 * g : 8 * g + 8, 0:32, :].reshape(256, 128)
        return jnp.concatenate([block, tails[8 * g : 8 * g + 8].reshape(256, 32)], axis=1)

    rows = group_rows(1)
    for q in range(4):
        chunk = jnp.dot(pick[256 * q : 256 * q + 256, 256:512], rows, preferred_element_type=F32)
        picked[256 * q : 256 * q + 256] = chunk.astype(BF16)

    for d in (0,) + NEAR_FIRST:
        arrive(ring[d])
        arrive(2 * RING + ring[d])
    rows = [group_rows(0), group_rows(2)]
    for q in range(4):
        part = pl.ds(256 * q, 256)
        chunk = [
            jnp.dot(pick[part, 512 * u : 512 * u + 256], rows[u], preferred_element_type=F32).astype(BF16)
            for u in range(2)
        ]
        picked[part] = picked[part] + chunk[0] + chunk[1]
    remote(mine, trans.at[pl.ds((1 - core) * half, half)], pair_send, pair_recv, sibling).wait_recv()

    chosen = lax.broadcasted_iota(jnp.int32, (16, 80, 128), 2) // 8 == lax.broadcasted_iota(jnp.int32, (16, 80, 128), 0)
    for q in range(8):
        blocks = trans[16 * q : 16 * q + 16].reshape(1280, 160)
        every = lax.dot_general(blocks, picked[128 * q : 128 * q + 128], NT, preferred_element_type=F32)
        every = jnp.where(chosen, every.reshape(16, 80, 128), 0.0).sum(axis=0)
        contrib[:, 128 * q : 128 * q + 128] = every.astype(BF16)

    near[...] = lax.dot_general(place[...], contrib[...], NT, preferred_element_type=F32).astype(BF16)
    load_m.wait()

    for j in range(16):
        rows = near[16 * j : 16 * j + 16, :]
        for u in range(2):
            both = jnp.dot(rows, tmat[2 * j + u], preferred_element_type=F32)
            scat[2 * j + u] = both[8 * u : 8 * u + 8]

    for y in range(RING):
        h, r = y // 4, 2 * (y % 4)
        rows = jnp.concatenate([scat[16 * h : 16 * h + 16, r + u, :] for u in range(2)], axis=0)
        parts[y] = packed_rows(rows).astype(BF16)
    for d in FAR_FIRST:
        start(remote(parts.at[ring[d]], sums.at[here], send_out.at[d], recv_out.at[here], at(ring[d])))
    total = parts[here].astype(F32)
    for d in NEAR_FIRST:
        y = ring[d]
        remote(parts.at[y], sums.at[y], send_out.at[d], recv_out.at[y], sibling).wait_recv()
        total = total + sums[y].astype(F32)
    whole = jnp.concatenate([total[0:32], tail_rows(total[32:40])], axis=1)
    out[...] = (coeffs[...].astype(F32) - whole.reshape(2, 16, 160)).astype(BF16)
    for copy in sends:
        copy.wait_send()


def solution(mesh):
    groups = mesh.shape["gx"]

    def step(coeffs, translations, tmatrix, pair_target, pair_source, pair_count):
        half = translations.shape[0]
        hbm = pl.BlockSpec(memory_space=pltpu.HBM)
        return pl.pallas_call(
            functools.partial(kernel, groups),
            out_shape=pltpu.VMEM(coeffs.shape, BF16),
            in_specs=[pl.BlockSpec(memory_space=pltpu.SMEM)] + [hbm] * 5,
            out_specs=pl.BlockSpec(memory_space=pltpu.VMEM),
            scratch_shapes=[
                pltpu.SMEM(pair_target.shape, jnp.int32),
                pltpu.SMEM(pair_source.shape, jnp.int32),
                pltpu.VMEM(coeffs.shape, BF16),
                pltpu.VMEM((2 * half, 80, 160), BF16),
                pltpu.VMEM((32, 80, 160), BF16),
                pltpu.VMEM((24, 48, 128), BF16),
                pltpu.VMEM((24, 32, 32), BF16),
                pltpu.VMEM((1024, 768), BF16),
                pltpu.VMEM((256, 1024), BF16),
                pltpu.VMEM((1024, 160), BF16),
                pltpu.VMEM((80, 1024), BF16),
                pltpu.VMEM((256, 80), BF16),
                pltpu.VMEM((32, 8, 160), F32),
                pltpu.VMEM((8, 48, 128), BF16),
                pltpu.VMEM((8, 48, 128), BF16),
                pltpu.SemaphoreType.DMA((5,)),
                pltpu.SemaphoreType.DMA((8,)),
                pltpu.SemaphoreType.DMA((16,)),
                pltpu.SemaphoreType.DMA((24,)),
                pltpu.SemaphoreType.DMA,
                pltpu.SemaphoreType.DMA,
                pltpu.SemaphoreType.DMA((8,)),
                pltpu.SemaphoreType.DMA((8,)),
            ],
            compiler_params=pltpu.CompilerParams(
                collective_id=0, has_side_effects=True, vmem_limit_bytes=67_000_000
            ),
        )(pair_count, pair_target, pair_source, coeffs, translations, tmatrix)

    placed = (
        P("gz", ("gx", "gy"), None),
        P(("gx", "gz"), "gy", None),
        P("gx", "gy", None),
        P("gx"),
        P("gx"),
        P("gx"),
    )
    return jax.shard_map(
        step, mesh=mesh, in_specs=placed, out_specs=P("gz", ("gx", "gy"), None), check_vma=False
    )
```

```python
import functools

import jax
import jax.numpy as jnp
from jax import lax
from jax.experimental import pallas as pl
from jax.experimental.pallas import tpu as pltpu
from jax.sharding import PartitionSpec as P

MESH = pl.DeviceIdType.MESH
F32 = jnp.float32
BF16 = jnp.bfloat16
NT = (((1,), (1,)), ((), ()))
RING = 8
NEAR_FIRST = (1, 7, 2, 6, 3, 5, 4)
FAR_FIRST = (4, 3, 5, 2, 6, 1, 7)


def packed_rows(rows):
    tails = [rows[8 * j : 8 * j + 8, 128:160] for j in range(4)]
    tail = jnp.concatenate(tails, axis=1)
    return jnp.concatenate([rows[:, :128], tail, jnp.zeros_like(tail)], axis=0)


def tail_rows(tail):
    return jnp.concatenate([tail[:, 32 * j : 32 * j + 32] for j in range(4)], axis=0)


def kernel(
    groups, count, target_hbm, source_hbm, coeffs_hbm, trans_hbm, tmat_hbm, out,
    target, source, coeffs, trans, tmat, win, tails, pick, place, picked, contrib, near, scat, parts, sums,
    local_sem, ready, send_one, recv_y, recv_z, pair_send, pair_recv, send_out, recv_out,
):
    load_c = pltpu.make_async_copy(coeffs_hbm, coeffs, local_sem.at[0])
    load_c.start()

    gx, gy, gz = lax.axis_index("gx"), lax.axis_index("gy"), lax.axis_index("gz")
    quarter, core = gz // 2, gz % 2
    here = gy * 4 + quarter
    half = trans_hbm.shape[0]
    pairs = 2 * half
    above, below = (gx + 1) % groups, (gx + groups - 1) % groups
    first, last = gx % RING == 0, gx % RING == RING - 1
    sibling = {"gx": gx, "gy": gy, "gz": quarter * 2 + 1 - core}
    ring = [(here + d) % RING for d in range(RING)]

    def at(group, y, c):
        return {"gx": group, "gy": y // 4, "gz": (y % 4) * 2 + c}

    barrier = pltpu.get_barrier_semaphore()

    def greet(peer):
        pl.semaphore_signal(barrier, inc=1, device_id=peer, device_id_type=MESH)

    greet(at(above, here, 0))
    greet(at(below, here, 0))
    greet(sibling)
    for d in FAR_FIRST:
        greet(at(gx, ring[d], 1))

    @pl.when(first)
    def _():
        for d in FAR_FIRST:
            greet(at(below, ring[d], 0))

    load_p = [
        pltpu.make_async_copy(target_hbm, target, local_sem.at[3]),
        pltpu.make_async_copy(source_hbm, source, local_sem.at[4]),
    ]
    load_t = pltpu.make_async_copy(trans_hbm, trans.at[pl.ds(core * half, half)], local_sem.at[1])
    load_m = pltpu.make_async_copy(tmat_hbm, tmat, local_sem.at[2])
    for load in load_p:
        load.start()
    load_t.start()
    load_m.start()

    load_c.wait()
    own = coeffs[...].astype(F32).reshape(32, 160)
    win[RING + here] = packed_rows(own).astype(BF16)

    def remote(src, dst, s, r, peer):
        return pltpu.make_async_remote_copy(
            src_ref=src, dst_ref=dst, send_sem=s, recv_sem=r, device_id=peer, device_id_type=MESH
        )

    def send_up(y, to):
        remote(win.at[RING + y], win.at[y], send_one, recv_z.at[0], at(above, to, core)).start()

    def send_down(y):
        remote(win.at[RING + y], win.at[2 * RING + y], send_one, recv_z.at[1], at(below, here, core)).start()

    def forward(y):
        @pl.when(jnp.logical_not(last))
        def _():
            send_up(y, here)

        send_down(y)

    def tell_sibling():
        pl.semaphore_signal(ready, inc=1, device_id=sibling, device_id_type=MESH)

    def enter_z():
        @pl.when(core == 0)
        def _():
            pl.semaphore_wait(barrier, jnp.where(last, 3 + 2 * RING, 5))
            tell_sibling()

        @pl.when(core == 1)
        def _():
            pl.semaphore_wait(ready, 1)

    @pl.when(jnp.logical_not(first))
    def _():
        enter_z()

        @pl.when(last)
        def _():
            for d in FAR_FIRST + (0,):
                send_up(here, ring[d])

        forward(here)

    @pl.when(core == 1)
    def _():
        pl.semaphore_wait(barrier, 1 + 2 * (RING - 1))
        tell_sibling()

    @pl.when(core == 0)
    def _():
        pl.semaphore_wait(ready, 1)

    for d in FAR_FIRST:
        remote(
            win.at[RING + here], win.at[RING + here], send_one, recv_y.at[RING - d], at(gx, ring[d], core)
        ).start()
    load_t.wait()
    mine = trans.at[pl.ds(core * half, half)]
    send_pair = remote(mine, mine, pair_send, pair_recv, sibling)
    send_pair.start()

    def unpack(slot):
        tail = tail_rows(win[slot, 32:48, :].astype(F32)[0:8])
        tails[slot] = tail.astype(BF16)

    def received(blocks, sem):
        remote(blocks, blocks, send_one, sem, sibling).wait_recv()

    for load in load_p:
        load.wait()
    lane = lax.broadcasted_iota(jnp.int32, (8, 128), 1)
    sub = lax.broadcasted_iota(jnp.int32, (8, 128), 0)
    diagonal = lane - 16 * sub

    def build_pick(j, carry):
        for v in range(4):
            codes = []
            for u in range(2):
                s = source[quarter * pairs + 8 * j + 2 * v + u]
                relative = (s // 32 - gx + 1 + groups) % groups
                codes.append((relative * 2 + (s % 32) // 16) * 1024 + s % 16)
            rows = pl.ds(pl.multiple_of(64 * j + 16 * v, 16), 16)
            for t in range(6):
                hot = [jnp.where(diagonal == c - 1024 * t, 1.0, 0.0) for c in codes]
                pick[rows, 128 * t : 128 * t + 128] = jnp.concatenate(hot, axis=0).astype(BF16)
        return carry

    lax.fori_loop(0, pairs // 8, build_pick, 0)

    for d in NEAR_FIRST:
        received(win.at[RING + ring[d]], recv_y.at[d])

        @pl.when(jnp.logical_not(first))
        def _():
            forward(ring[d])

    def build_place(q, carry):
        v = jnp.full((8, 128), -1, jnp.int32)
        for i in range(16):
            slot = quarter * pairs + q * 16 + i
            t = jnp.where(slot < count[0], target[slot], -1)
            v = jnp.where((lane // 8 == i) & (lane % 8 == sub), t, v)
        for s in range(16):
            hot = [jnp.where(v == 2 * s + u, 1.0, 0.0) for u in range(2)]
            place[16 * s : 16 * s + 16, pl.ds(pl.multiple_of(128 * q, 128), 128)] = jnp.concatenate(hot, axis=0).astype(BF16)
        return carry

    lax.fori_loop(0, pairs // 16, build_place, 0)

    def group_rows(g):
        for y in range(RING):
            unpack(RING * g + y)
        block = win[8 * g : 8 * g + 8, 0:32, :].reshape(256, 128)
        return jnp.concatenate([block, tails[8 * g : 8 * g + 8].reshape(256, 32)], axis=1)

    rows = group_rows(1)
    for q in range(4):
        chunk = jnp.dot(pick[256 * q : 256 * q + 256, 256:512], rows, preferred_element_type=F32)
        picked[256 * q : 256 * q + 256] = chunk.astype(BF16)

    @pl.when(first)
    def _():
        enter_z()
        for d in (0,) + NEAR_FIRST:
            send_up(ring[d], here)
            send_down(ring[d])

    for g, sem in ((2, 1), (0, 0)):
        received(win.at[8 * g : 8 * g + 8], recv_z.at[sem])
        rows = group_rows(g)
        for q in range(4):
            part = pl.ds(256 * q, 256)
            chunk = jnp.dot(pick[part, 256 * g : 256 * g + 256], rows, preferred_element_type=F32)
            picked[part] = picked[part] + chunk.astype(BF16)
    remote(mine, trans.at[pl.ds((1 - core) * half, half)], pair_send, pair_recv, sibling).wait_recv()

    chosen = lax.broadcasted_iota(jnp.int32, (16, 80, 128), 2) // 8 == lax.broadcasted_iota(jnp.int32, (16, 80, 128), 0)
    for q in range(8):
        blocks = trans[16 * q : 16 * q + 16].reshape(1280, 160)
        every = lax.dot_general(blocks, picked[128 * q : 128 * q + 128], NT, preferred_element_type=F32)
        every = jnp.where(chosen, every.reshape(16, 80, 128), 0.0).sum(axis=0)
        contrib[:, 128 * q : 128 * q + 128] = every.astype(BF16)

    near[...] = lax.dot_general(place[...], contrib[...], NT, preferred_element_type=F32).astype(BF16)
    load_m.wait()

    for j in range(16):
        rows = near[16 * j : 16 * j + 16, :]
        for u in range(2):
            both = jnp.dot(rows, tmat[2 * j + u], preferred_element_type=F32)
            scat[2 * j + u] = both[8 * u : 8 * u + 8]

    for y in range(RING):
        h, r = y // 4, 2 * (y % 4)
        rows = jnp.concatenate([scat[16 * h : 16 * h + 16, r + u, :] for u in range(2)], axis=0)
        parts[y] = packed_rows(rows).astype(BF16)
    for d in FAR_FIRST:
        remote(parts.at[ring[d]], sums.at[here], send_out, recv_out, at(gx, ring[d], core)).start()
    sums[here] = parts[here]
    remote(parts.at[0:7], sums.at[0:7], send_out, recv_out, sibling).wait_recv()
    total = sums[...].astype(F32).sum(axis=0)
    whole = jnp.concatenate([total[0:32], tail_rows(total[32:40])], axis=1)
    out[...] = (coeffs[...].astype(F32) - whole.reshape(2, 16, 160)).astype(BF16)
    remote(win.at[0:23], win.at[0:23], send_one, recv_y.at[0], sibling).wait_send()

    remote(parts.at[0:7], sums.at[0:7], send_out, recv_out, sibling).wait_send()
    send_pair.wait_send()


def solution(mesh):
    groups = mesh.shape["gx"]

    def step(coeffs, translations, tmatrix, pair_target, pair_source, pair_count):
        half = translations.shape[0]
        hbm = pl.BlockSpec(memory_space=pltpu.HBM)
        return pl.pallas_call(
            functools.partial(kernel, groups),
            out_shape=pltpu.VMEM(coeffs.shape, BF16),
            in_specs=[pl.BlockSpec(memory_space=pltpu.SMEM)] + [hbm] * 5,
            out_specs=pl.BlockSpec(memory_space=pltpu.VMEM),
            scratch_shapes=[
                pltpu.SMEM(pair_target.shape, jnp.int32),
                pltpu.SMEM(pair_source.shape, jnp.int32),
                pltpu.VMEM(coeffs.shape, BF16),
                pltpu.VMEM((2 * half, 80, 160), BF16),
                pltpu.VMEM((32, 80, 160), BF16),
                pltpu.VMEM((24, 48, 128), BF16),
                pltpu.VMEM((24, 32, 32), BF16),
                pltpu.VMEM((1024, 768), BF16),
                pltpu.VMEM((256, 1024), BF16),
                pltpu.VMEM((1024, 160), BF16),
                pltpu.VMEM((80, 1024), BF16),
                pltpu.VMEM((256, 80), BF16),
                pltpu.VMEM((32, 8, 160), F32),
                pltpu.VMEM((8, 48, 128), BF16),
                pltpu.VMEM((8, 48, 128), BF16),
                pltpu.SemaphoreType.DMA((5,)),
                pltpu.SemaphoreType.REGULAR,
                pltpu.SemaphoreType.DMA,
                pltpu.SemaphoreType.DMA((8,)),
                pltpu.SemaphoreType.DMA((2,)),
                pltpu.SemaphoreType.DMA,
                pltpu.SemaphoreType.DMA,
                pltpu.SemaphoreType.DMA,
                pltpu.SemaphoreType.DMA,
            ],
            compiler_params=pltpu.CompilerParams(
                collective_id=0, has_side_effects=True, vmem_limit_bytes=67_000_000
            ),
        )(pair_count, pair_target, pair_source, coeffs, translations, tmatrix)

    placed = (
        P("gz", ("gx", "gy"), None),
        P(("gx", "gz"), "gy", None),
        P("gx", "gy", None),
        P("gx"),
        P("gx"),
        P("gx"),
    )
    return jax.shard_map(
        step, mesh=mesh, in_specs=placed, out_specs=P("gz", ("gx", "gy"), None), check_vma=False
    )
```

```python
import functools

import jax
import jax.numpy as jnp
from jax import lax
from jax.experimental import pallas as pl
from jax.experimental.pallas import tpu as pltpu
from jax.sharding import PartitionSpec as P

MESH = pl.DeviceIdType.MESH
F32 = jnp.float32
BF16 = jnp.bfloat16
NT = (((1,), (1,)), ((), ()))
RING = 8
NEAR_FIRST = (1, 7, 2, 6, 3, 5, 4)
FAR_FIRST = (4, 3, 5, 2, 6, 1, 7)


def packed_rows(rows):
    tails = [rows[8 * j : 8 * j + 8, 128:160] for j in range(4)]
    tail = jnp.concatenate(tails, axis=1)
    return jnp.concatenate([rows[:, :128], tail], axis=0)


def tail_rows(tail):
    return jnp.concatenate([tail[:, 32 * j : 32 * j + 32] for j in range(4)], axis=0)


def kernel(
    groups, count, target_hbm, source_hbm, coeffs_hbm, trans_hbm, tmat_hbm, out,
    target, source, coeffs, trans, tmat, win, tails, ends_of, keep, pick, place, picked, near, scat, parts, sums,
    local_sem, ready, send_one, recv_y, recv_z, pair_send, pair_recv, send_out, recv_out,
):
    load_c = pltpu.make_async_copy(coeffs_hbm, coeffs, local_sem.at[0])
    load_c.start()

    gx, gy, gz = lax.axis_index("gx"), lax.axis_index("gy"), lax.axis_index("gz")
    quarter, core = gz // 2, gz % 2
    here = gy * 4 + quarter
    half = trans_hbm.shape[0]
    pairs = 2 * half
    above, below = (gx + 1) % groups, (gx + groups - 1) % groups
    first, last = gx % RING == 0, gx % RING == RING - 1
    lane = lax.broadcasted_iota(jnp.int32, (8, 128), 1)
    sub = lax.broadcasted_iota(jnp.int32, (8, 128), 0)
    sibling = {"gx": gx, "gy": gy, "gz": quarter * 2 + 1 - core}
    ring = [(here + d) % RING for d in range(RING)]

    def at(group, y, c):
        return {"gx": group, "gy": y // 4, "gz": (y % 4) * 2 + c}

    barrier = pltpu.get_barrier_semaphore()

    def greet(peer):
        pl.semaphore_signal(barrier, inc=1, device_id=peer, device_id_type=MESH)

    greet(at(above, here, 0))
    greet(at(below, here, 0))
    greet(sibling)
    for d in FAR_FIRST:
        greet(at(gx, ring[d], 1))

    @pl.when(first)
    def _():
        for d in FAR_FIRST:
            greet(at(below, ring[d], 0))

    load_p = [
        pltpu.make_async_copy(target_hbm, target, local_sem.at[3]),
        pltpu.make_async_copy(source_hbm, source, local_sem.at[4]),
    ]
    load_t = pltpu.make_async_copy(trans_hbm, trans.at[pl.ds(core * half, half)], local_sem.at[1])
    load_m = pltpu.make_async_copy(tmat_hbm, tmat, local_sem.at[2])
    for load in load_p:
        load.start()
    load_t.start()
    load_m.start()

    load_c.wait()
    own = coeffs[...].astype(F32).reshape(32, 160)
    win[RING + here] = packed_rows(own).astype(BF16)

    def remote(src, dst, s, r, peer):
        return pltpu.make_async_remote_copy(
            src_ref=src, dst_ref=dst, send_sem=s, recv_sem=r, device_id=peer, device_id_type=MESH
        )

    def send_up(y, to):
        remote(win.at[RING + y], win.at[y], send_one, recv_z.at[0], at(above, to, core)).start()

    def send_down(y):
        remote(win.at[RING + y], win.at[2 * RING + y], send_one, recv_z.at[1], at(below, here, core)).start()

    def forward(y):
        @pl.when(jnp.logical_not(last))
        def _():
            send_up(y, here)

        send_down(y)

    def tell_sibling():
        pl.semaphore_signal(ready, inc=1, device_id=sibling, device_id_type=MESH)

    def enter_z():
        @pl.when(core == 0)
        def _():
            pl.semaphore_wait(barrier, jnp.where(last, 3 + 2 * RING, 5))
            tell_sibling()

        @pl.when(core == 1)
        def _():
            pl.semaphore_wait(ready, 1)

    @pl.when(jnp.logical_not(first))
    def _():
        enter_z()

        @pl.when(last)
        def _():
            for d in FAR_FIRST + (0,):
                send_up(here, ring[d])

        forward(here)

    @pl.when(core == 1)
    def _():
        pl.semaphore_wait(barrier, 1 + 2 * (RING - 1))
        tell_sibling()

    @pl.when(core == 0)
    def _():
        pl.semaphore_wait(ready, 1)

    for d in FAR_FIRST:
        remote(
            win.at[RING + here], win.at[RING + here], send_one, recv_y.at[RING - d], at(gx, ring[d], core)
        ).start()
    load_t.wait()
    mine = trans.at[pl.ds(core * half, half)]
    send_pair = remote(mine, mine, pair_send, pair_recv, sibling)
    send_pair.start()

    def unpack(slot):
        packed = win[slot, 32:40, :].astype(F32)
        rows = []
        for j in range(4):
            tail = jnp.where(lane // 32 == j, packed, 0.0)
            tail = tail + pltpu.roll(tail, 32, 1)
            rows.append(tail + pltpu.roll(tail, 64, 1))
        tails[slot] = jnp.concatenate(rows, axis=0).astype(BF16)

    def received(blocks, sem):
        remote(blocks, blocks, send_one, sem, sibling).wait_recv()

    for load in load_p:
        load.wait()
    diagonal = lane - 16 * sub

    def build_pick(j, carry):
        for v in range(4):
            codes = []
            for u in range(2):
                s = source[quarter * pairs + 8 * j + 2 * v + u]
                relative = (s // 32 - gx + 1 + groups) % groups
                codes.append((relative * 2 + (s % 32) // 16) * 1024 + s % 16)
            rows = pl.ds(pl.multiple_of(64 * j + 16 * v, 16), 16)
            for t in range(6):
                hot = [jnp.where(diagonal == c - 1024 * t, 1.0, 0.0) for c in codes]
                pick[rows, 128 * t : 128 * t + 128] = jnp.concatenate(hot, axis=0).astype(BF16)
        return carry

    lax.fori_loop(0, pairs // 8, build_pick, 0)

    for d in NEAR_FIRST:
        received(win.at[RING + ring[d]], recv_y.at[d])

        @pl.when(jnp.logical_not(first))
        def _():
            forward(ring[d])

    def pack_tails(m, carry):
        ends = [trans[8 * m + i, :, 128:160] for i in range(8)]
        ends_of[m] = jnp.concatenate(ends, axis=1)
        return carry

    lax.fori_loop(core * 8, core * 8 + 8, pack_tails, 0)

    def build_place(q, carry):
        v = jnp.full((8, 128), -1, jnp.int32)
        for i in range(16):
            slot = quarter * pairs + q * 16 + i
            t = jnp.where(slot < count[0], target[slot], -1)
            v = jnp.where((lane // 8 == i) & (lane % 8 == sub), t, v)
        for s in range(16):
            hot = [jnp.where(v == 2 * s + u, 1.0, 0.0) for u in range(2)]
            place[16 * s : 16 * s + 16, pl.ds(pl.multiple_of(128 * q, 128), 128)] = jnp.concatenate(hot, axis=0).astype(BF16)
        return carry

    lax.fori_loop(0, pairs // 16, build_place, 0)

    def group_rows(g):
        for y in range(RING):
            unpack(RING * g + y)
        block = win[8 * g : 8 * g + 8, 0:32, :].reshape(256, 128)
        return jnp.concatenate([block, tails[8 * g : 8 * g + 8].reshape(256, 128)], axis=1)

    pair_of = lax.broadcasted_iota(jnp.int32, (128, 128), 0) // 8
    column = lax.broadcasted_iota(jnp.int32, (128, 128), 1)
    for u, mask in enumerate((
        pair_of % 2 == 0, pair_of % 2 == 1, pair_of % 8 == column // 32, pair_of % 8 == column // 32 + 4,
    )):
        keep[u] = jnp.where(mask, 1.0, 0.0).astype(BF16)

    rows = group_rows(1)
    for q in range(4):
        chunk = jnp.dot(pick[256 * q : 256 * q + 256, 256:512], rows, preferred_element_type=F32)
        picked[256 * q : 256 * q + 256] = chunk.astype(BF16)

    @pl.when(first)
    def _():
        enter_z()
        for d in (0,) + NEAR_FIRST:
            send_up(ring[d], here)
            send_down(ring[d])

    remote(mine, trans.at[pl.ds((1 - core) * half, half)], pair_send, pair_recv, sibling).wait_recv()
    lax.fori_loop(8 - core * 8, 16 - core * 8, pack_tails, 0)

    def pick_more(g, c):
        part = pl.ds(256 * c, 256)
        chunk = jnp.dot(pick[part, 256 * g : 256 * g + 256], rows, preferred_element_type=F32)
        return picked[part] + chunk.astype(BF16)

    received(win.at[16:24], recv_z.at[1])
    rows = group_rows(2)
    for c in range(4):
        picked[256 * c : 256 * c + 256] = pick_more(2, c)

    load_m.wait()
    received(win.at[0:8], recv_z.at[0])
    rows = group_rows(0)
    lane_of = lax.broadcasted_iota(jnp.int32, (80, 128), 1)
    sums_at = None
    for c in range(4):
        both = pick_more(0, c)
        contrib = []
        for v in range(2):
            q = 2 * c + v
            mains, ends = both[128 * v : 128 * v + 128, 0:128], both[128 * v : 128 * v + 128, 128:256]
            blocks = [
                jnp.concatenate([trans[16 * q + 2 * j, :, 0:128], trans[16 * q + 2 * j + 1, :, 0:128]], axis=1)
                for j in range(8)
            ]
            main = lax.dot_general(
                jnp.concatenate(blocks, axis=0),
                jnp.concatenate([mains * keep[0], mains * keep[1]], axis=1),
                NT,
                preferred_element_type=F32,
            )
            end = lax.dot_general(
                ends_of[2 * q : 2 * q + 2].reshape(160, 256),
                jnp.concatenate([ends * keep[2], ends * keep[3]], axis=1),
                NT,
                preferred_element_type=F32,
            )
            total = jnp.where(lane_of < 64, end[0:80], end[80:160])
            half_sum = main[0:80]
            for j in range(1, 8):
                half_sum = jnp.where(lane_of // 16 == j, main[80 * j : 80 * j + 80], half_sum)
            contrib.append((total + half_sum).astype(BF16))
        part = lax.dot_general(
            place[:, 256 * c : 256 * c + 256], jnp.concatenate(contrib, axis=1), NT, preferred_element_type=F32
        )
        sums_at = part if sums_at is None else sums_at + part
    near[...] = sums_at.astype(BF16)

    for j in range(16):
        rows = near[16 * j : 16 * j + 16, :]
        for u in range(2):
            both = jnp.dot(rows, tmat[2 * j + u], preferred_element_type=F32)
            scat[2 * j + u] = both[8 * u : 8 * u + 8]

    for y in range(RING):
        h, r = y // 4, 2 * (y % 4)
        rows = jnp.concatenate([scat[16 * h : 16 * h + 16, r + u, :] for u in range(2)], axis=0)
        parts[y] = packed_rows(rows).astype(BF16)
    for d in FAR_FIRST:
        remote(parts.at[ring[d]], sums.at[here], send_out, recv_out, at(gx, ring[d], core)).start()
    sums[here] = parts[here]
    remote(parts.at[0:7], sums.at[0:7], send_out, recv_out, sibling).wait_recv()
    total = sums[...].astype(F32).sum(axis=0)
    whole = jnp.concatenate([total[0:32], tail_rows(total[32:40])], axis=1)
    out[...] = (coeffs[...].astype(F32) - whole.reshape(2, 16, 160)).astype(BF16)
    remote(win.at[0:23], win.at[0:23], send_one, recv_y.at[0], sibling).wait_send()

    remote(parts.at[0:7], sums.at[0:7], send_out, recv_out, sibling).wait_send()
    send_pair.wait_send()


def solution(mesh):
    groups = mesh.shape["gx"]

    def step(coeffs, translations, tmatrix, pair_target, pair_source, pair_count):
        half = translations.shape[0]
        hbm = pl.BlockSpec(memory_space=pltpu.HBM)
        return pl.pallas_call(
            functools.partial(kernel, groups),
            out_shape=pltpu.VMEM(coeffs.shape, BF16),
            in_specs=[pl.BlockSpec(memory_space=pltpu.SMEM)] + [hbm] * 5,
            out_specs=pl.BlockSpec(memory_space=pltpu.VMEM),
            scratch_shapes=[
                pltpu.SMEM(pair_target.shape, jnp.int32),
                pltpu.SMEM(pair_source.shape, jnp.int32),
                pltpu.VMEM(coeffs.shape, BF16),
                pltpu.VMEM((2 * half, 80, 160), BF16),
                pltpu.VMEM((32, 80, 160), BF16),
                pltpu.VMEM((24, 40, 128), BF16),
                pltpu.VMEM((24, 32, 128), BF16),
                pltpu.VMEM((16, 80, 256), BF16),
                pltpu.VMEM((4, 128, 128), BF16),
                pltpu.VMEM((1024, 768), BF16),
                pltpu.VMEM((256, 1024), BF16),
                pltpu.VMEM((1024, 256), BF16),
                pltpu.VMEM((256, 80), BF16),
                pltpu.VMEM((32, 8, 160), F32),
                pltpu.VMEM((8, 40, 128), BF16),
                pltpu.VMEM((8, 40, 128), BF16),
                pltpu.SemaphoreType.DMA((5,)),
                pltpu.SemaphoreType.REGULAR,
                pltpu.SemaphoreType.DMA,
                pltpu.SemaphoreType.DMA((8,)),
                pltpu.SemaphoreType.DMA((2,)),
                pltpu.SemaphoreType.DMA,
                pltpu.SemaphoreType.DMA,
                pltpu.SemaphoreType.DMA,
                pltpu.SemaphoreType.DMA,
            ],
            compiler_params=pltpu.CompilerParams(
                collective_id=0, has_side_effects=True, vmem_limit_bytes=67_000_000
            ),
        )(pair_count, pair_target, pair_source, coeffs, translations, tmatrix)

    placed = (
        P("gz", ("gx", "gy"), None),
        P(("gx", "gz"), "gy", None),
        P("gx", "gy", None),
        P("gx"),
        P("gx"),
        P("gx"),
    )
    return jax.shard_map(
        step, mesh=mesh, in_specs=placed, out_specs=P("gz", ("gx", "gy"), None), check_vma=False
    )
```

```python
import functools

import jax
import jax.numpy as jnp
from jax import lax
from jax.experimental import pallas as pl
from jax.experimental.pallas import tpu as pltpu
from jax.sharding import PartitionSpec as P

MESH = pl.DeviceIdType.MESH
F32 = jnp.float32
BF16 = jnp.bfloat16
NT = (((1,), (1,)), ((), ()))
RING = 8
NEAR_FIRST = (1, 7, 2, 6, 3, 5, 4)
FAR_FIRST = (4, 3, 5, 2, 6, 1, 7)


def packed_rows(rows):
    tails = [rows[8 * j : 8 * j + 8, 128:160] for j in range(4)]
    tail = jnp.concatenate(tails, axis=1)
    return jnp.concatenate([rows[:, :128], tail], axis=0)


def tail_rows(tail):
    return jnp.concatenate([tail[:, 32 * j : 32 * j + 32] for j in range(4)], axis=0)


def kernel(
    groups, count, target_hbm, source_hbm, coeffs_hbm, trans_hbm, tmat_hbm, out,
    target, source, coeffs, trans, tmat, win, tails, ends_of, keep, pick, place, picked, near, scat, parts, sums,
    local_sem, ready, send_one, recv_y, recv_z, pair_send, pair_recv, send_out, recv_out,
):
    load_c = pltpu.make_async_copy(coeffs_hbm, coeffs, local_sem.at[0])
    load_c.start()

    gx, gy, gz = lax.axis_index("gx"), lax.axis_index("gy"), lax.axis_index("gz")
    quarter, core = gz // 2, gz % 2
    here = gy * 4 + quarter
    half = trans_hbm.shape[0]
    pairs = 2 * half
    above, below = (gx + 1) % groups, (gx + groups - 1) % groups
    first, last = gx % RING == 0, gx % RING == RING - 1
    lane = lax.broadcasted_iota(jnp.int32, (8, 128), 1)
    sub = lax.broadcasted_iota(jnp.int32, (8, 128), 0)
    sibling = {"gx": gx, "gy": gy, "gz": quarter * 2 + 1 - core}
    ring = [(here + d) % RING for d in range(RING)]

    def at(group, y, c):
        return {"gx": group, "gy": y // 4, "gz": (y % 4) * 2 + c}

    barrier = pltpu.get_barrier_semaphore()

    def greet(peer):
        pl.semaphore_signal(barrier, inc=1, device_id=peer, device_id_type=MESH)

    greet(at(above, here, 0))
    greet(at(below, here, 0))
    greet(sibling)
    for d in FAR_FIRST:
        greet(at(gx, ring[d], 1))

    @pl.when(first)
    def _():
        for d in FAR_FIRST:
            greet(at(below, ring[d], 0))

    load_p = [
        pltpu.make_async_copy(target_hbm, target, local_sem.at[3]),
        pltpu.make_async_copy(source_hbm, source, local_sem.at[4]),
    ]
    load_t = pltpu.make_async_copy(trans_hbm, trans.at[pl.ds(core * half, half)], local_sem.at[1])
    load_m = pltpu.make_async_copy(tmat_hbm, tmat, local_sem.at[2])
    for load in load_p:
        load.start()
    load_t.start()
    load_m.start()

    def tell_sibling():
        pl.semaphore_signal(ready, inc=1, device_id=sibling, device_id_type=MESH)

    def hear_z():
        @pl.when(core == 0)
        def _():
            pl.semaphore_wait(barrier, jnp.where(last, 3 + 2 * RING, 5))
            tell_sibling()

    @pl.when(jnp.logical_not(first))
    def _():
        hear_z()

    load_c.wait()
    own = coeffs[...].astype(F32).reshape(32, 160)
    win[RING + here] = packed_rows(own).astype(BF16)

    def remote(src, dst, s, r, peer):
        return pltpu.make_async_remote_copy(
            src_ref=src, dst_ref=dst, send_sem=s, recv_sem=r, device_id=peer, device_id_type=MESH
        )

    def send_up(y, to):
        remote(win.at[RING + y], win.at[y], send_one, recv_z.at[0], at(above, to, core)).start()

    def send_down(y):
        remote(win.at[RING + y], win.at[2 * RING + y], send_one, recv_z.at[1], at(below, here, core)).start()

    def forward(y):
        @pl.when(jnp.logical_not(last))
        def _():
            send_up(y, here)

        send_down(y)

    @pl.when(jnp.logical_not(first))
    def _():
        @pl.when(core == 1)
        def _():
            pl.semaphore_wait(ready, 1)

        @pl.when(last)
        def _():
            for d in FAR_FIRST + (0,):
                send_up(here, ring[d])

        forward(here)

    @pl.when(core == 1)
    def _():
        pl.semaphore_wait(barrier, 1 + 2 * (RING - 1))
        tell_sibling()

    @pl.when(core == 0)
    def _():
        pl.semaphore_wait(ready, 1)

    for d in FAR_FIRST:
        remote(
            win.at[RING + here], win.at[RING + here], send_one, recv_y.at[RING - d], at(gx, ring[d], core)
        ).start()
    load_t.wait()
    mine = trans.at[pl.ds(core * half, half)]
    send_pair = remote(mine, mine, pair_send, pair_recv, sibling)
    send_pair.start()

    def unpack(slot):
        packed = win[slot, 32:40, :].astype(F32)
        rows = []
        for j in range(4):
            tail = jnp.where(lane // 32 == j, packed, 0.0)
            tail = tail + pltpu.roll(tail, 32, 1)
            rows.append(tail + pltpu.roll(tail, 64, 1))
        tails[slot] = jnp.concatenate(rows, axis=0).astype(BF16)

    def received(blocks, sem):
        remote(blocks, blocks, send_one, sem, sibling).wait_recv()

    for load in load_p:
        load.wait()
    diagonal = lane - 16 * sub

    def build_pick(j, carry):
        for v in range(4):
            codes = []
            for u in range(2):
                s = source[quarter * pairs + 8 * j + 2 * v + u]
                relative = (s // 32 - gx + 1 + groups) % groups
                codes.append((relative * 2 + (s % 32) // 16) * 1024 + s % 16)
            rows = pl.ds(pl.multiple_of(64 * j + 16 * v, 16), 16)
            for t in range(6):
                hot = [jnp.where(diagonal == c - 1024 * t, 1.0, 0.0) for c in codes]
                pick[rows, 128 * t : 128 * t + 128] = jnp.concatenate(hot, axis=0).astype(BF16)
        return carry

    lax.fori_loop(0, pairs // 8, build_pick, 0)

    for d in NEAR_FIRST:
        received(win.at[RING + ring[d]], recv_y.at[d])

        @pl.when(jnp.logical_not(first))
        def _():
            forward(ring[d])

    def pack_tails(m, carry):
        ends = [trans[8 * m + i, :, 128:160] for i in range(8)]
        ends_of[m] = jnp.concatenate(ends, axis=1)
        return carry

    lax.fori_loop(core * 8, core * 8 + 8, pack_tails, 0)

    def build_place(q, carry):
        v = jnp.full((8, 128), -1, jnp.int32)
        for i in range(16):
            slot = quarter * pairs + q * 16 + i
            t = jnp.where(slot < count[0], target[slot], -1)
            v = jnp.where((lane // 8 == i) & (lane % 8 == sub), t, v)
        for s in range(16):
            hot = [jnp.where(v == 2 * s + u, 1.0, 0.0) for u in range(2)]
            place[16 * s : 16 * s + 16, pl.ds(pl.multiple_of(128 * q, 128), 128)] = jnp.concatenate(hot, axis=0).astype(BF16)
        return carry

    lax.fori_loop(0, pairs // 16, build_place, 0)

    def group_rows(g):
        for y in range(RING):
            unpack(RING * g + y)
        block = win[8 * g : 8 * g + 8, 0:32, :].reshape(256, 128)
        return jnp.concatenate([block, tails[8 * g : 8 * g + 8].reshape(256, 128)], axis=1)

    pair_of = lax.broadcasted_iota(jnp.int32, (128, 128), 0) // 8
    column = lax.broadcasted_iota(jnp.int32, (128, 128), 1)
    for u, mask in enumerate((
        pair_of % 2 == 0, pair_of % 2 == 1, pair_of % 8 == column // 32, pair_of % 8 == column // 32 + 4,
    )):
        keep[u] = jnp.where(mask, 1.0, 0.0).astype(BF16)

    rows = group_rows(1)
    for q in range(4):
        chunk = jnp.dot(pick[256 * q : 256 * q + 256, 256:512], rows, preferred_element_type=F32)
        picked[256 * q : 256 * q + 256] = chunk.astype(BF16)

    @pl.when(first)
    def _():
        hear_z()

        @pl.when(core == 1)
        def _():
            pl.semaphore_wait(ready, 1)

        for d in (0,) + NEAR_FIRST:
            send_up(ring[d], here)
            send_down(ring[d])

    remote(mine, trans.at[pl.ds((1 - core) * half, half)], pair_send, pair_recv, sibling).wait_recv()
    lax.fori_loop(8 - core * 8, 16 - core * 8, pack_tails, 0)

    def pick_more(g, c):
        part = pl.ds(256 * c, 256)
        chunk = jnp.dot(pick[part, 256 * g : 256 * g + 256], rows, preferred_element_type=F32)
        return picked[part] + chunk.astype(BF16)

    received(win.at[16:24], recv_z.at[1])
    rows = group_rows(2)
    for c in range(4):
        picked[256 * c : 256 * c + 256] = pick_more(2, c)

    load_m.wait()
    received(win.at[0:8], recv_z.at[0])
    rows = group_rows(0)
    lane_of = lax.broadcasted_iota(jnp.int32, (80, 128), 1)
    sums_at = None
    for c in range(4):
        both = pick_more(0, c)
        contrib = []
        for v in range(2):
            q = 2 * c + v
            mains, ends = both[128 * v : 128 * v + 128, 0:128], both[128 * v : 128 * v + 128, 128:256]
            blocks = [
                jnp.concatenate([trans[16 * q + 2 * j, :, 0:128], trans[16 * q + 2 * j + 1, :, 0:128]], axis=1)
                for j in range(8)
            ]
            main = lax.dot_general(
                jnp.concatenate(blocks, axis=0),
                jnp.concatenate([mains * keep[0], mains * keep[1]], axis=1),
                NT,
                preferred_element_type=F32,
            )
            end = lax.dot_general(
                ends_of[2 * q : 2 * q + 2].reshape(160, 256),
                jnp.concatenate([ends * keep[2], ends * keep[3]], axis=1),
                NT,
                preferred_element_type=F32,
            )
            total = jnp.where(lane_of < 64, end[0:80], end[80:160])
            half_sum = main[0:80]
            for j in range(1, 8):
                half_sum = jnp.where(lane_of // 16 == j, main[80 * j : 80 * j + 80], half_sum)
            contrib.append((total + half_sum).astype(BF16))
        part = lax.dot_general(
            place[:, 256 * c : 256 * c + 256], jnp.concatenate(contrib, axis=1), NT, preferred_element_type=F32
        )
        sums_at = part if sums_at is None else sums_at + part
    near[...] = sums_at.astype(BF16)

    for j in range(16):
        rows = near[16 * j : 16 * j + 16, :]
        for u in range(2):
            both = jnp.dot(rows, tmat[2 * j + u], preferred_element_type=F32)
            scat[2 * j + u] = both[8 * u : 8 * u + 8]

    for y in range(RING):
        h, r = y // 4, 2 * (y % 4)
        rows = jnp.concatenate([scat[16 * h : 16 * h + 16, r + u, :] for u in range(2)], axis=0)
        parts[y] = packed_rows(rows).astype(BF16)
    for d in FAR_FIRST:
        remote(parts.at[ring[d]], sums.at[here], send_out, recv_out, at(gx, ring[d], core)).start()
    sums[here] = parts[here]
    remote(parts.at[0:7], sums.at[0:7], send_out, recv_out, sibling).wait_recv()
    total = sums[...].astype(F32).sum(axis=0)
    whole = jnp.concatenate([total[0:32], tail_rows(total[32:40])], axis=1)
    out[...] = (coeffs[...].astype(F32) - whole.reshape(2, 16, 160)).astype(BF16)
    remote(win.at[0:23], win.at[0:23], send_one, recv_y.at[0], sibling).wait_send()

    remote(parts.at[0:7], sums.at[0:7], send_out, recv_out, sibling).wait_send()
    send_pair.wait_send()


def solution(mesh):
    groups = mesh.shape["gx"]

    def step(coeffs, translations, tmatrix, pair_target, pair_source, pair_count):
        half = translations.shape[0]
        hbm = pl.BlockSpec(memory_space=pltpu.HBM)
        return pl.pallas_call(
            functools.partial(kernel, groups),
            out_shape=pltpu.VMEM(coeffs.shape, BF16),
            in_specs=[pl.BlockSpec(memory_space=pltpu.SMEM)] + [hbm] * 5,
            out_specs=pl.BlockSpec(memory_space=pltpu.VMEM),
            scratch_shapes=[
                pltpu.SMEM(pair_target.shape, jnp.int32),
                pltpu.SMEM(pair_source.shape, jnp.int32),
                pltpu.VMEM(coeffs.shape, BF16),
                pltpu.VMEM((2 * half, 80, 160), BF16),
                pltpu.VMEM((32, 80, 160), BF16),
                pltpu.VMEM((24, 40, 128), BF16),
                pltpu.VMEM((24, 32, 128), BF16),
                pltpu.VMEM((16, 80, 256), BF16),
                pltpu.VMEM((4, 128, 128), BF16),
                pltpu.VMEM((1024, 768), BF16),
                pltpu.VMEM((256, 1024), BF16),
                pltpu.VMEM((1024, 256), BF16),
                pltpu.VMEM((256, 80), BF16),
                pltpu.VMEM((32, 8, 160), F32),
                pltpu.VMEM((8, 40, 128), BF16),
                pltpu.VMEM((8, 40, 128), BF16),
                pltpu.SemaphoreType.DMA((5,)),
                pltpu.SemaphoreType.REGULAR,
                pltpu.SemaphoreType.DMA,
                pltpu.SemaphoreType.DMA((8,)),
                pltpu.SemaphoreType.DMA((2,)),
                pltpu.SemaphoreType.DMA,
                pltpu.SemaphoreType.DMA,
                pltpu.SemaphoreType.DMA,
                pltpu.SemaphoreType.DMA,
            ],
            compiler_params=pltpu.CompilerParams(
                collective_id=0, has_side_effects=True, vmem_limit_bytes=67_000_000
            ),
        )(pair_count, pair_target, pair_source, coeffs, translations, tmatrix)

    placed = (
        P("gz", ("gx", "gy"), None),
        P(("gx", "gz"), "gy", None),
        P("gx", "gy", None),
        P("gx"),
        P("gx"),
        P("gx"),
    )
    return jax.shard_map(
        step, mesh=mesh, in_specs=placed, out_specs=P("gz", ("gx", "gy"), None), check_vma=False
    )
```

```python
import functools

import jax
import jax.numpy as jnp
from jax import lax
from jax.experimental import pallas as pl
from jax.experimental.pallas import tpu as pltpu
from jax.sharding import PartitionSpec as P

MESH = pl.DeviceIdType.MESH
F32 = jnp.float32
BF16 = jnp.bfloat16
NT = (((1,), (1,)), ((), ()))
RING = 8
NEAR_FIRST = (1, 7, 2, 6, 3, 5, 4)
FAR_FIRST = (4, 3, 5, 2, 6, 1, 7)


def packed_rows(rows):
    tails = [rows[8 * j : 8 * j + 8, 128:160] for j in range(4)]
    tail = jnp.concatenate(tails, axis=1)
    return jnp.concatenate([rows[:, :128], tail], axis=0)


def tail_rows(tail):
    return jnp.concatenate([tail[:, 32 * j : 32 * j + 32] for j in range(4)], axis=0)


def kernel(
    groups, count, target_hbm, source_hbm, coeffs_hbm, trans_hbm, tmat_hbm, out,
    target, source, coeffs, trans, tmat, win, tails, ends_of, keep, pick, place, picked, wide, scat, parts, sums,
    local_sem, ready, send_one, recv_y, recv_z, pair_send, pair_recv, send_out, recv_out,
):
    load_c = pltpu.make_async_copy(coeffs_hbm, coeffs, local_sem.at[0])
    load_c.start()

    gx, gy, gz = lax.axis_index("gx"), lax.axis_index("gy"), lax.axis_index("gz")
    quarter, core = gz // 2, gz % 2
    here = gy * 4 + quarter
    half = trans_hbm.shape[0]
    pairs = 2 * half
    above, below = (gx + 1) % groups, (gx + groups - 1) % groups
    first, last = gx % RING == 0, gx % RING == RING - 1
    lane = lax.broadcasted_iota(jnp.int32, (8, 128), 1)
    sub = lax.broadcasted_iota(jnp.int32, (8, 128), 0)
    sibling = {"gx": gx, "gy": gy, "gz": quarter * 2 + 1 - core}
    ring = [(here + d) % RING for d in range(RING)]

    def at(group, y, c):
        return {"gx": group, "gy": y // 4, "gz": (y % 4) * 2 + c}

    barrier = pltpu.get_barrier_semaphore()

    def greet(peer):
        pl.semaphore_signal(barrier, inc=1, device_id=peer, device_id_type=MESH)

    greet(at(above, here, 0))
    greet(at(below, here, 0))
    greet(sibling)
    for d in FAR_FIRST:
        greet(at(gx, ring[d], 1))

    @pl.when(first)
    def _():
        for d in FAR_FIRST:
            greet(at(below, ring[d], 0))

    load_p = [
        pltpu.make_async_copy(target_hbm, target, local_sem.at[3]),
        pltpu.make_async_copy(source_hbm, source, local_sem.at[4]),
    ]
    load_t = pltpu.make_async_copy(trans_hbm, trans.at[pl.ds(core * half, half)], local_sem.at[1])
    load_m = pltpu.make_async_copy(tmat_hbm, tmat, local_sem.at[2])
    for load in load_p:
        load.start()
    load_t.start()
    load_m.start()

    def tell_sibling():
        pl.semaphore_signal(ready, inc=1, device_id=sibling, device_id_type=MESH)

    def hear_z():
        @pl.when(core == 0)
        def _():
            pl.semaphore_wait(barrier, jnp.where(last, 3 + 2 * RING, 5))
            tell_sibling()

    @pl.when(jnp.logical_not(first))
    def _():
        hear_z()

    load_c.wait()
    own = coeffs[...].astype(F32).reshape(32, 160)
    win[RING + here] = packed_rows(own).astype(BF16)

    def remote(src, dst, s, r, peer):
        return pltpu.make_async_remote_copy(
            src_ref=src, dst_ref=dst, send_sem=s, recv_sem=r, device_id=peer, device_id_type=MESH
        )

    def send_up(y, to):
        remote(win.at[RING + y], win.at[y], send_one, recv_z.at[0], at(above, to, core)).start()

    def send_down(y):
        remote(win.at[RING + y], win.at[2 * RING + y], send_one, recv_z.at[1], at(below, here, core)).start()

    def forward(y):
        @pl.when(jnp.logical_not(last))
        def _():
            send_up(y, here)

        send_down(y)

    @pl.when(jnp.logical_not(first))
    def _():
        @pl.when(core == 1)
        def _():
            pl.semaphore_wait(ready, 1)

        @pl.when(last)
        def _():
            for d in FAR_FIRST + (0,):
                send_up(here, ring[d])

        forward(here)

    @pl.when(core == 1)
    def _():
        pl.semaphore_wait(barrier, 1 + 2 * (RING - 1))
        tell_sibling()

    @pl.when(core == 0)
    def _():
        pl.semaphore_wait(ready, 1)

    for d in FAR_FIRST:
        remote(
            win.at[RING + here], win.at[RING + here], send_one, recv_y.at[RING - d], at(gx, ring[d], core)
        ).start()
    load_t.wait()
    mine = trans.at[pl.ds(core * half, half)]
    send_pair = remote(mine, mine, pair_send, pair_recv, sibling)
    send_pair.start()

    def unpack(slot):
        packed = win[slot, 32:40, :].astype(F32)
        turned = [packed] + [pltpu.roll(packed, 32 * j, 1) for j in range(1, 4)]
        rows = []
        for j in range(4):
            tail = turned[(3 - j) % 4]
            for v in range(3):
                tail = jnp.where(lane // 32 == v, turned[(v - j) % 4], tail)
            rows.append(tail)
        tails[slot] = jnp.concatenate(rows, axis=0).astype(BF16)

    def received(blocks, sem):
        remote(blocks, blocks, send_one, sem, sibling).wait_recv()

    for load in load_p:
        load.wait()
    diagonal = lane - 16 * sub

    def build_pick(j, carry):
        for v in range(4):
            codes = []
            for u in range(2):
                s = source[quarter * pairs + 8 * j + 2 * v + u]
                relative = (s // 32 - gx + 1 + groups) % groups
                codes.append((relative * 2 + (s % 32) // 16) * 1024 + s % 16)
            rows = pl.ds(pl.multiple_of(64 * j + 16 * v, 16), 16)
            for t in range(6):
                hot = [jnp.where(diagonal == c - 1024 * t, 1.0, 0.0) for c in codes]
                pick[rows, 128 * t : 128 * t + 128] = jnp.concatenate(hot, axis=0).astype(BF16)
        return carry

    lax.fori_loop(0, pairs // 8, build_pick, 0)

    def pack_tails(m, carry):
        ends = [trans[8 * m + i, :, 128:160] for i in range(8)]
        ends_of[m] = jnp.concatenate(ends, axis=1)
        return carry

    def repeat_ends(m, carry):
        for u in range(4):
            block = tmat[4 * m + u]
            wide[4 * m + u] = jnp.concatenate([block[:, 0:128]] + [block[:, 128:160]] * 4, axis=1)
        return carry

    def build_place(q, carry):
        v = jnp.full((8, 128), -1, jnp.int32)
        for i in range(16):
            slot = quarter * pairs + q * 16 + i
            t = jnp.where(slot < count[0], target[slot], -1)
            v = jnp.where((lane // 8 == i) & (lane % 8 == sub), t, v)
        for s in range(16):
            hot = [jnp.where(v == 2 * s + u, 1.0, 0.0) for u in range(2)]
            place[16 * s : 16 * s + 16, pl.ds(pl.multiple_of(128 * q, 128), 128)] = jnp.concatenate(hot, axis=0).astype(BF16)
        return carry

    def prepare():
        lax.fori_loop(core * 8, core * 8 + 8, pack_tails, 0)
        load_m.wait()
        lax.fori_loop(0, 8, repeat_ends, 0)
        lax.fori_loop(0, pairs // 16, build_place, 0)

    @pl.when(first)
    def _():
        prepare()

    for d in NEAR_FIRST:
        received(win.at[RING + ring[d]], recv_y.at[d])

        @pl.when(jnp.logical_not(first))
        def _():
            forward(ring[d])

    @pl.when(jnp.logical_not(first))
    def _():
        prepare()

    def group_rows(g):
        for y in range(RING):
            unpack(RING * g + y)
        block = win[8 * g : 8 * g + 8, 0:32, :].reshape(256, 128)
        return jnp.concatenate([block, tails[8 * g : 8 * g + 8].reshape(256, 128)], axis=1)

    pair_of = lax.broadcasted_iota(jnp.int32, (128, 128), 0) // 8
    column = lax.broadcasted_iota(jnp.int32, (128, 128), 1)
    for u, mask in enumerate((
        pair_of % 2 == 0, pair_of % 2 == 1, pair_of % 8 == column // 32, pair_of % 8 == column // 32 + 4,
    )):
        keep[u] = jnp.where(mask, 1.0, 0.0).astype(BF16)

    rows = group_rows(1)
    for q in range(4):
        chunk = jnp.dot(pick[256 * q : 256 * q + 256, 256:512], rows, preferred_element_type=F32)
        picked[256 * q : 256 * q + 256] = chunk.astype(BF16)

    @pl.when(first)
    def _():
        hear_z()

        @pl.when(core == 1)
        def _():
            pl.semaphore_wait(ready, 1)

        for d in (0,) + NEAR_FIRST:
            send_up(ring[d], here)
            send_down(ring[d])

    remote(mine, trans.at[pl.ds((1 - core) * half, half)], pair_send, pair_recv, sibling).wait_recv()
    lax.fori_loop(8 - core * 8, 16 - core * 8, pack_tails, 0)

    def pick_more(g, c):
        part = pl.ds(256 * c, 256)
        chunk = jnp.dot(pick[part, 256 * g : 256 * g + 256], rows, preferred_element_type=F32)
        return picked[part] + chunk.astype(BF16)

    received(win.at[16:24], recv_z.at[1])
    rows = group_rows(2)
    for c in range(4):
        picked[256 * c : 256 * c + 256] = pick_more(2, c)

    received(win.at[0:8], recv_z.at[0])
    rows = group_rows(0)
    lane_of = lax.broadcasted_iota(jnp.int32, (80, 128), 1)
    sums_at = None
    for c in range(4):
        both = pick_more(0, c)
        contrib = []
        for v in range(2):
            q = 2 * c + v
            mains, ends = both[128 * v : 128 * v + 128, 0:128], both[128 * v : 128 * v + 128, 128:256]
            blocks = [
                jnp.concatenate([trans[16 * q + 2 * j, :, 0:128], trans[16 * q + 2 * j + 1, :, 0:128]], axis=1)
                for j in range(8)
            ]
            main = lax.dot_general(
                jnp.concatenate(blocks, axis=0),
                jnp.concatenate([mains * keep[0], mains * keep[1]], axis=1),
                NT,
                preferred_element_type=F32,
            )
            end = lax.dot_general(
                ends_of[2 * q : 2 * q + 2].reshape(160, 256),
                jnp.concatenate([ends * keep[2], ends * keep[3]], axis=1),
                NT,
                preferred_element_type=F32,
            )
            total = jnp.where(lane_of < 64, end[0:80], end[80:160])
            half_sum = main[0:80]
            for j in range(1, 8):
                half_sum = jnp.where(lane_of // 16 == j, main[80 * j : 80 * j + 80], half_sum)
            contrib.append((total + half_sum).astype(BF16))
        part = lax.dot_general(
            place[:, 256 * c : 256 * c + 256], jnp.concatenate(contrib, axis=1), NT, preferred_element_type=F32
        )
        sums_at = part if sums_at is None else sums_at + part
    near = sums_at.astype(BF16)

    for j in range(16):
        for u in range(2):
            both = jnp.dot(near[16 * j : 16 * j + 16], wide[2 * j + u], preferred_element_type=F32)
            scat[2 * j + u] = both[8 * u : 8 * u + 8]

    for y in range(RING):
        h, r = 16 * (y // 4), 2 * (y % 4)
        rows = [scat[h : h + 16, r + u, 0:128] for u in range(2)]
        ends = [scat[h + 8 * (j % 2) : h + 8 * (j % 2) + 8, r + j // 2, 128:256] for j in range(4)]
        tail = ends[3]
        for v in range(3):
            tail = jnp.where(lane // 32 == v, ends[v], tail)
        parts[y] = jnp.concatenate(rows + [tail], axis=0).astype(BF16)
    for d in FAR_FIRST:
        remote(parts.at[ring[d]], sums.at[here], send_out, recv_out, at(gx, ring[d], core)).start()
    sums[here] = parts[here]
    remote(parts.at[0:7], sums.at[0:7], send_out, recv_out, sibling).wait_recv()
    total = sums[...].astype(F32).sum(axis=0)
    whole = jnp.concatenate([total[0:32], tail_rows(total[32:40])], axis=1)
    out[...] = (coeffs[...].astype(F32) - whole.reshape(2, 16, 160)).astype(BF16)
    remote(win.at[0:23], win.at[0:23], send_one, recv_y.at[0], sibling).wait_send()

    remote(parts.at[0:7], sums.at[0:7], send_out, recv_out, sibling).wait_send()
    send_pair.wait_send()


def solution(mesh):
    groups = mesh.shape["gx"]

    def step(coeffs, translations, tmatrix, pair_target, pair_source, pair_count):
        half = translations.shape[0]
        hbm = pl.BlockSpec(memory_space=pltpu.HBM)
        return pl.pallas_call(
            functools.partial(kernel, groups),
            out_shape=pltpu.VMEM(coeffs.shape, BF16),
            in_specs=[pl.BlockSpec(memory_space=pltpu.SMEM)] + [hbm] * 5,
            out_specs=pl.BlockSpec(memory_space=pltpu.VMEM),
            scratch_shapes=[
                pltpu.SMEM(pair_target.shape, jnp.int32),
                pltpu.SMEM(pair_source.shape, jnp.int32),
                pltpu.VMEM(coeffs.shape, BF16),
                pltpu.VMEM((2 * half, 80, 160), BF16),
                pltpu.VMEM((32, 80, 160), BF16),
                pltpu.VMEM((24, 40, 128), BF16),
                pltpu.VMEM((24, 32, 128), BF16),
                pltpu.VMEM((16, 80, 256), BF16),
                pltpu.VMEM((4, 128, 128), BF16),
                pltpu.VMEM((1024, 768), BF16),
                pltpu.VMEM((256, 1024), BF16),
                pltpu.VMEM((1024, 256), BF16),
                pltpu.VMEM((32, 80, 256), BF16),
                pltpu.VMEM((32, 8, 256), F32),
                pltpu.VMEM((8, 40, 128), BF16),
                pltpu.VMEM((8, 40, 128), BF16),
                pltpu.SemaphoreType.DMA((5,)),
                pltpu.SemaphoreType.REGULAR,
                pltpu.SemaphoreType.DMA,
                pltpu.SemaphoreType.DMA((8,)),
                pltpu.SemaphoreType.DMA((2,)),
                pltpu.SemaphoreType.DMA,
                pltpu.SemaphoreType.DMA,
                pltpu.SemaphoreType.DMA,
                pltpu.SemaphoreType.DMA,
            ],
            compiler_params=pltpu.CompilerParams(
                collective_id=0, has_side_effects=True, vmem_limit_bytes=67_000_000
            ),
        )(pair_count, pair_target, pair_source, coeffs, translations, tmatrix)

    placed = (
        P("gz", ("gx", "gy"), None),
        P(("gx", "gz"), "gy", None),
        P("gx", "gy", None),
        P("gx"),
        P("gx"),
        P("gx"),
    )
    return jax.shard_map(
        step, mesh=mesh, in_specs=placed, out_specs=P("gz", ("gx", "gy"), None), check_vma=False
    )
```

```python
import functools

import jax
import jax.numpy as jnp
from jax import lax
from jax.experimental import pallas as pl
from jax.experimental.pallas import tpu as pltpu
from jax.sharding import PartitionSpec as P

MESH = pl.DeviceIdType.MESH
F32 = jnp.float32
BF16 = jnp.bfloat16
NT = (((1,), (1,)), ((), ()))
RING = 8
NEAR_FIRST = (1, 7, 2, 6, 3, 5, 4)
FAR_FIRST = (4, 3, 5, 2, 6, 1, 7)


def packed_rows(rows):
    tails = [rows[8 * j : 8 * j + 8, 128:160] for j in range(4)]
    tail = jnp.concatenate(tails, axis=1)
    return jnp.concatenate([rows[:, :128], tail], axis=0)


def tail_rows(tail):
    return jnp.concatenate([tail[:, 32 * j : 32 * j + 32] for j in range(4)], axis=0)


def kernel(
    groups, count, target_hbm, source_hbm, coeffs_hbm, trans_hbm, tmat_hbm, out,
    target, source, coeffs, trans, tmat, win, window, ends_of, place, wide, scat, parts, sums,
    local_sem, ready, send_one, recv_y, recv_z, pair_send, pair_recv, send_out, recv_out,
):
    load_c = pltpu.make_async_copy(coeffs_hbm, coeffs, local_sem.at[0])
    load_c.start()

    gx, gy, gz = lax.axis_index("gx"), lax.axis_index("gy"), lax.axis_index("gz")
    quarter, core = gz // 2, gz % 2
    here = gy * 4 + quarter
    half = trans_hbm.shape[0]
    pairs = 2 * half
    above, below = (gx + 1) % groups, (gx + groups - 1) % groups
    first, last = gx % RING == 0, gx % RING == RING - 1
    lane = lax.broadcasted_iota(jnp.int32, (8, 128), 1)
    sub = lax.broadcasted_iota(jnp.int32, (8, 128), 0)
    sibling = {"gx": gx, "gy": gy, "gz": quarter * 2 + 1 - core}
    ring = [(here + d) % RING for d in range(RING)]

    def at(group, y, c):
        return {"gx": group, "gy": y // 4, "gz": (y % 4) * 2 + c}

    barrier = pltpu.get_barrier_semaphore()

    def greet(peer):
        pl.semaphore_signal(barrier, inc=1, device_id=peer, device_id_type=MESH)

    greet(at(above, here, 0))
    greet(at(below, here, 0))
    greet(sibling)
    for d in FAR_FIRST:
        greet(at(gx, ring[d], 1))

    @pl.when(first)
    def _():
        for d in FAR_FIRST:
            greet(at(below, ring[d], 0))

    load_p = [
        pltpu.make_async_copy(target_hbm, target, local_sem.at[3]),
        pltpu.make_async_copy(source_hbm, source, local_sem.at[4]),
    ]
    load_t = pltpu.make_async_copy(trans_hbm, trans.at[pl.ds(core * half, half)], local_sem.at[1])
    load_m = pltpu.make_async_copy(tmat_hbm, tmat, local_sem.at[2])
    for load in load_p:
        load.start()
    load_t.start()
    load_m.start()

    def tell_sibling():
        pl.semaphore_signal(ready, inc=1, device_id=sibling, device_id_type=MESH)

    def hear_z():
        @pl.when(core == 0)
        def _():
            pl.semaphore_wait(barrier, jnp.where(last, 3 + 2 * RING, 5))
            tell_sibling()

    @pl.when(jnp.logical_not(first))
    def _():
        hear_z()

    load_c.wait()
    own = coeffs[...].astype(F32).reshape(32, 160)
    win[RING + here] = packed_rows(own).astype(BF16)

    def remote(src, dst, s, r, peer):
        return pltpu.make_async_remote_copy(
            src_ref=src, dst_ref=dst, send_sem=s, recv_sem=r, device_id=peer, device_id_type=MESH
        )

    def send_up(y, to):
        remote(win.at[RING + y], win.at[y], send_one, recv_z.at[0], at(above, to, core)).start()

    def send_down(y):
        remote(win.at[RING + y], win.at[2 * RING + y], send_one, recv_z.at[1], at(below, here, core)).start()

    def forward(y):
        @pl.when(jnp.logical_not(last))
        def _():
            send_up(y, here)

        send_down(y)

    @pl.when(jnp.logical_not(first))
    def _():
        @pl.when(core == 1)
        def _():
            pl.semaphore_wait(ready, 1)

        @pl.when(last)
        def _():
            for d in FAR_FIRST + (0,):
                send_up(here, ring[d])

        forward(here)

    @pl.when(core == 1)
    def _():
        pl.semaphore_wait(barrier, 1 + 2 * (RING - 1))
        tell_sibling()

    @pl.when(core == 0)
    def _():
        pl.semaphore_wait(ready, 1)

    for d in FAR_FIRST:
        remote(
            win.at[RING + here], win.at[RING + here], send_one, recv_y.at[RING - d], at(gx, ring[d], core)
        ).start()
    load_t.wait()
    mine = trans.at[pl.ds(core * half, half)]
    send_pair = remote(mine, mine, pair_send, pair_recv, sibling)
    send_pair.start()

    def unpack(group):
        for y in range(RING):
            block = win[RING * group + y].astype(F32)
            base, r = 32 * group + 16 * (y // 4), 2 * (y % 4)
            packed = block[32:40]
            turned = [packed] + [pltpu.roll(packed, 32 * j, 1) for j in range(1, 4)]
            for j in range(4):
                tail = turned[(3 - j) % 4]
                for v in range(3):
                    tail = jnp.where(lane // 32 == v, turned[(v - j) % 4], tail)
                rows = pl.ds(base + 8 * (j % 2), 8)
                window[rows, r + j // 2, 0:128] = block[8 * j : 8 * j + 8]
                window[rows, r + j // 2, 128:256] = tail

    def received(blocks, sem):
        remote(blocks, blocks, send_one, sem, sibling).wait_recv()

    def pack_tails(m, carry):
        ends = [trans[8 * m + i, :, 128:160] for i in range(8)]
        ends_of[m] = jnp.concatenate(ends, axis=1)
        return carry

    def repeat_ends(m, carry):
        for u in range(4):
            block = tmat[4 * m + u]
            wide[4 * m + u] = jnp.concatenate([block[:, 0:128]] + [block[:, 128:160]] * 4, axis=1)
        return carry

    def build_place(q, carry):
        v = jnp.full((8, 128), -1, jnp.int32)
        for i in range(16):
            slot = quarter * pairs + q * 16 + i
            t = jnp.where(slot < count[0], target[slot], -1)
            v = jnp.where((lane // 8 == i) & (lane % 8 == sub), t, v)
        for s in range(16):
            hot = [jnp.where(v == 2 * s + u, 1.0, 0.0) for u in range(2)]
            place[16 * s : 16 * s + 16, pl.ds(pl.multiple_of(128 * q, 128), 128)] = jnp.concatenate(hot, axis=0).astype(BF16)
        return carry

    def prepare():
        for load in load_p:
            load.wait()
        lax.fori_loop(core * 8, core * 8 + 8, pack_tails, 0)
        load_m.wait()
        lax.fori_loop(0, 8, repeat_ends, 0)
        lax.fori_loop(0, pairs // 16, build_place, 0)

    @pl.when(first)
    def _():
        prepare()

    for d in NEAR_FIRST:
        received(win.at[RING + ring[d]], recv_y.at[d])

        @pl.when(jnp.logical_not(first))
        def _():
            forward(ring[d])

    @pl.when(jnp.logical_not(first))
    def _():
        prepare()

    def group_rows(g):
        for y in range(RING):
            unpack(RING * g + y)
        block = win[8 * g : 8 * g + 8, 0:32, :].reshape(256, 128)
        return jnp.concatenate([block, tails[8 * g : 8 * g + 8].reshape(256, 128)], axis=1)

    unpack(1)

    @pl.when(first)
    def _():
        hear_z()

        @pl.when(core == 1)
        def _():
            pl.semaphore_wait(ready, 1)

        for d in (0,) + NEAR_FIRST:
            send_up(ring[d], here)
            send_down(ring[d])

    remote(mine, trans.at[pl.ds((1 - core) * half, half)], pair_send, pair_recv, sibling).wait_recv()
    lax.fori_loop(8 - core * 8, 16 - core * 8, pack_tails, 0)

    received(win.at[16:24], recv_z.at[1])
    unpack(2)
    spheres = 32 * groups
    shift = spheres + 32 - 32 * gx
    nothing = jnp.zeros((8, 128), F32)

    def picked_rows(q):
        mains, ends = [], []
        for i in range(0, 16, 2):
            pair = []
            for u in range(2):
                s = source[quarter * pairs + 16 * q + i + u]
                pair.append(window[jnp.minimum(lax.rem(s + shift, spheres), 95)])
            mains += [
                jnp.concatenate([pair[0][:, 0:128], nothing], axis=1),
                jnp.concatenate([nothing, pair[1][:, 0:128]], axis=1),
            ]
            for u in range(2):
                end = jnp.where(lane // 32 == (i + u) % 4, pair[u][:, 128:256], 0.0)
                ends.append(jnp.concatenate([end, nothing] if i % 8 < 4 else [nothing, end], axis=1))
        return jnp.concatenate(mains, axis=0).astype(BF16), jnp.concatenate(ends, axis=0).astype(BF16)

    received(win.at[0:8], recv_z.at[0])
    unpack(0)
    lane_of = lax.broadcasted_iota(jnp.int32, (80, 128), 1)
    sums_at = None
    for c in range(4):
        contrib = []
        for v in range(2):
            q = 2 * c + v
            mains, ends = picked_rows(q)
            blocks = [
                jnp.concatenate([trans[16 * q + 2 * j, :, 0:128], trans[16 * q + 2 * j + 1, :, 0:128]], axis=1)
                for j in range(8)
            ]
            main = lax.dot_general(
                jnp.concatenate(blocks, axis=0),
                mains,
                NT,
                preferred_element_type=F32,
            )
            end = lax.dot_general(
                ends_of[2 * q : 2 * q + 2].reshape(160, 256),
                ends,
                NT,
                preferred_element_type=F32,
            )
            total = jnp.where(lane_of < 64, end[0:80], end[80:160])
            half_sum = main[0:80]
            for j in range(1, 8):
                half_sum = jnp.where(lane_of // 16 == j, main[80 * j : 80 * j + 80], half_sum)
            contrib.append((total + half_sum).astype(BF16))
        part = lax.dot_general(
            place[:, 256 * c : 256 * c + 256], jnp.concatenate(contrib, axis=1), NT, preferred_element_type=F32
        )
        sums_at = part if sums_at is None else sums_at + part
    near = sums_at.astype(BF16)

    for j in range(16):
        for u in range(2):
            both = jnp.dot(near[16 * j : 16 * j + 16], wide[2 * j + u], preferred_element_type=F32)
            scat[2 * j + u] = both[8 * u : 8 * u + 8]

    for y in range(RING):
        h, r = 16 * (y // 4), 2 * (y % 4)
        rows = [scat[h : h + 16, r + u, 0:128] for u in range(2)]
        ends = [scat[h + 8 * (j % 2) : h + 8 * (j % 2) + 8, r + j // 2, 128:256] for j in range(4)]
        tail = ends[3]
        for v in range(3):
            tail = jnp.where(lane // 32 == v, ends[v], tail)
        parts[y] = jnp.concatenate(rows + [tail], axis=0).astype(BF16)
    for d in FAR_FIRST:
        remote(parts.at[ring[d]], sums.at[here], send_out, recv_out, at(gx, ring[d], core)).start()
    sums[here] = parts[here]
    remote(parts.at[0:7], sums.at[0:7], send_out, recv_out, sibling).wait_recv()
    total = sums[...].astype(F32).sum(axis=0)
    whole = jnp.concatenate([total[0:32], tail_rows(total[32:40])], axis=1)
    out[...] = (coeffs[...].astype(F32) - whole.reshape(2, 16, 160)).astype(BF16)
    remote(win.at[0:23], win.at[0:23], send_one, recv_y.at[0], sibling).wait_send()

    remote(parts.at[0:7], sums.at[0:7], send_out, recv_out, sibling).wait_send()
    send_pair.wait_send()


def solution(mesh):
    groups = mesh.shape["gx"]

    def step(coeffs, translations, tmatrix, pair_target, pair_source, pair_count):
        half = translations.shape[0]
        hbm = pl.BlockSpec(memory_space=pltpu.HBM)
        return pl.pallas_call(
            functools.partial(kernel, groups),
            out_shape=pltpu.VMEM(coeffs.shape, BF16),
            in_specs=[pl.BlockSpec(memory_space=pltpu.SMEM)] + [hbm] * 5,
            out_specs=pl.BlockSpec(memory_space=pltpu.VMEM),
            scratch_shapes=[
                pltpu.SMEM(pair_target.shape, jnp.int32),
                pltpu.SMEM(pair_source.shape, jnp.int32),
                pltpu.VMEM(coeffs.shape, BF16),
                pltpu.VMEM((2 * half, 80, 160), BF16),
                pltpu.VMEM((32, 80, 160), BF16),
                pltpu.VMEM((24, 40, 128), BF16),
                pltpu.VMEM((96, 8, 256), F32),
                pltpu.VMEM((16, 80, 256), BF16),
                pltpu.VMEM((256, 1024), BF16),
                pltpu.VMEM((32, 80, 256), BF16),
                pltpu.VMEM((32, 8, 256), F32),
                pltpu.VMEM((8, 40, 128), BF16),
                pltpu.VMEM((8, 40, 128), BF16),
                pltpu.SemaphoreType.DMA((5,)),
                pltpu.SemaphoreType.REGULAR,
                pltpu.SemaphoreType.DMA,
                pltpu.SemaphoreType.DMA((8,)),
                pltpu.SemaphoreType.DMA((2,)),
                pltpu.SemaphoreType.DMA,
                pltpu.SemaphoreType.DMA,
                pltpu.SemaphoreType.DMA,
                pltpu.SemaphoreType.DMA,
            ],
            compiler_params=pltpu.CompilerParams(
                collective_id=0, has_side_effects=True, vmem_limit_bytes=67_000_000
            ),
        )(pair_count, pair_target, pair_source, coeffs, translations, tmatrix)

    placed = (
        P("gz", ("gx", "gy"), None),
        P(("gx", "gz"), "gy", None),
        P("gx", "gy", None),
        P("gx"),
        P("gx"),
        P("gx"),
    )
    return jax.shard_map(
        step, mesh=mesh, in_specs=placed, out_specs=P("gz", ("gx", "gy"), None), check_vma=False
    )
```

```python
import functools

import jax
import jax.numpy as jnp
from jax import lax
from jax.experimental import pallas as pl
from jax.experimental.pallas import tpu as pltpu
from jax.sharding import PartitionSpec as P

MESH = pl.DeviceIdType.MESH
F32 = jnp.float32
BF16 = jnp.bfloat16
NT = (((1,), (1,)), ((), ()))
RING = 8
NEAR_FIRST = (1, 7, 2, 6, 3, 5, 4)
FAR_FIRST = (4, 3, 5, 2, 6, 1, 7)


def packed_rows(rows):
    tails = [rows[8 * j : 8 * j + 8, 128:160] for j in range(4)]
    tail = jnp.concatenate(tails, axis=1)
    return jnp.concatenate([rows[:, :128], tail], axis=0)


def tail_rows(tail):
    return jnp.concatenate([tail[:, 32 * j : 32 * j + 32] for j in range(4)], axis=0)


def kernel(
    groups, count, target_hbm, source_hbm, coeffs_hbm, trans_hbm, tmat_hbm, out,
    target, source, coeffs, trans, tmat, win, window, ends_of, place, wide, scat, parts, sums,
    local_sem, ready, send_one, recv_y, recv_z, pair_send, pair_recv, send_out, recv_out,
):
    load_c = pltpu.make_async_copy(coeffs_hbm, coeffs, local_sem.at[0])
    load_c.start()

    gx, gy, gz = lax.axis_index("gx"), lax.axis_index("gy"), lax.axis_index("gz")
    quarter, core = gz // 2, gz % 2
    here = gy * 4 + quarter
    half = trans_hbm.shape[0]
    pairs = 2 * half
    above, below = (gx + 1) % groups, (gx + groups - 1) % groups
    first, last = gx % RING == 0, gx % RING == RING - 1
    lane = lax.broadcasted_iota(jnp.int32, (8, 128), 1)
    sub = lax.broadcasted_iota(jnp.int32, (8, 128), 0)
    sibling = {"gx": gx, "gy": gy, "gz": quarter * 2 + 1 - core}
    ring = [(here + d) % RING for d in range(RING)]

    def at(group, y, c):
        return {"gx": group, "gy": y // 4, "gz": (y % 4) * 2 + c}

    barrier = pltpu.get_barrier_semaphore()

    def greet(peer):
        pl.semaphore_signal(barrier, inc=1, device_id=peer, device_id_type=MESH)

    @pl.when(gx % RING == RING - 2)
    def _():
        greet(at(above, here, 1))

    @pl.when(gx % RING != RING - 2)
    def _():
        greet(at(above, here, 0))

    greet(at(below, here, 0))
    greet(sibling)
    for d in FAR_FIRST:
        greet(at(gx, ring[d], 1))

    @pl.when(first)
    def _():
        for d in FAR_FIRST:
            greet(at(below, ring[d], 0))

    load_p = [
        pltpu.make_async_copy(target_hbm, target, local_sem.at[3]),
        pltpu.make_async_copy(source_hbm, source, local_sem.at[4]),
    ]
    load_t = pltpu.make_async_copy(trans_hbm, trans.at[pl.ds(core * half, half)], local_sem.at[1])
    load_m = pltpu.make_async_copy(tmat_hbm, tmat, local_sem.at[2])
    for load in load_p:
        load.start()
    load_t.start()
    load_m.start()

    def tell_sibling():
        pl.semaphore_signal(ready, inc=1, device_id=sibling, device_id_type=MESH)

    def hear_z():
        @pl.when(core == 0)
        def _():
            pl.semaphore_wait(barrier, jnp.where(last, 1 + 2 * RING, 5))
            tell_sibling()

    @pl.when(jnp.logical_not(first))
    def _():
        hear_z()

    load_c.wait()
    own = coeffs[...].astype(F32).reshape(32, 160)
    win[RING + here] = packed_rows(own).astype(BF16)

    def remote(src, dst, s, r, peer):
        return pltpu.make_async_remote_copy(
            src_ref=src, dst_ref=dst, send_sem=s, recv_sem=r, device_id=peer, device_id_type=MESH
        )

    def send_up(y, to):
        remote(win.at[RING + y], win.at[y], send_one, recv_z.at[2 * (y // 4)], at(above, to, core)).start()

    def send_down(y):
        remote(win.at[RING + y], win.at[2 * RING + y], send_one, recv_z.at[1], at(below, here, core)).start()

    def forward(y):
        @pl.when(jnp.logical_not(last))
        def _():
            send_up(y, here)

        send_down(y)

    @pl.when(jnp.logical_not(first))
    def _():
        @pl.when(core == 1)
        def _():
            pl.semaphore_wait(ready, 1)

        @pl.when(last)
        def _():
            for d in FAR_FIRST + (0,):
                send_up(here, ring[d])

        @pl.when(jnp.logical_not(last))
        def _():
            forward(here)

    @pl.when(core == 1)
    def _():
        pl.semaphore_wait(barrier, jnp.where(last, 1 + 2 * RING, 2 * RING - 1))
        tell_sibling()

    @pl.when(core == 0)
    def _():
        pl.semaphore_wait(ready, 1)

    for d in FAR_FIRST:
        remote(
            win.at[RING + here], win.at[RING + here], send_one, recv_y.at[RING - d], at(gx, ring[d], core)
        ).start()

    @pl.when(last)
    def _():
        send_down(here)

    load_t.wait()
    mine = trans.at[pl.ds(core * half, half)]
    send_pair = remote(mine, mine, pair_send, pair_recv, sibling)
    send_pair.start()

    def unpack(group, blocks=range(RING)):
        for y in blocks:
            block = win[RING * group + y].astype(F32)
            base, r = 32 * group + 16 * (y // 4), 2 * (y % 4)
            packed = block[32:40]
            turned = [packed] + [pltpu.roll(packed, 32 * j, 1) for j in range(1, 4)]
            for j in range(4):
                tail = turned[(3 - j) % 4]
                for v in range(3):
                    tail = jnp.where(lane // 32 == v, turned[(v - j) % 4], tail)
                rows = pl.ds(base + 8 * (j % 2), 8)
                window[rows, r + j // 2, 0:128] = block[8 * j : 8 * j + 8]
                window[rows, r + j // 2, 128:256] = tail

    def received(blocks, sem):
        remote(blocks, blocks, send_one, sem, sibling).wait_recv()

    def pack_tails(m, carry):
        ends = [trans[8 * m + i, :, 128:160] for i in range(8)]
        ends_of[m] = jnp.concatenate(ends, axis=1)
        return carry

    def repeat_ends(m, carry):
        for u in range(4):
            block = tmat[4 * m + u]
            wide[4 * m + u] = jnp.concatenate([block[:, 0:128]] + [block[:, 128:160]] * 4, axis=1)
        return carry

    def build_place(q, carry):
        v = jnp.full((8, 128), -1, jnp.int32)
        for i in range(16):
            slot = quarter * pairs + q * 16 + i
            t = jnp.where(slot < count[0], target[slot], -1)
            v = jnp.where((lane // 8 == i) & (lane % 8 == sub), t, v)
        for s in range(16):
            hot = [jnp.where(v == 2 * s + u, 1.0, 0.0) for u in range(2)]
            place[16 * s : 16 * s + 16, pl.ds(pl.multiple_of(128 * q, 128), 128)] = jnp.concatenate(hot, axis=0).astype(BF16)
        return carry

    def prepare():
        for load in load_p:
            load.wait()
        lax.fori_loop(core * 8, core * 8 + 8, pack_tails, 0)
        load_m.wait()
        lax.fori_loop(0, 8, repeat_ends, 0)
        lax.fori_loop(0, pairs // 16, build_place, 0)

    @pl.when(first)
    def _():
        prepare()

    for d in NEAR_FIRST:
        received(win.at[RING + ring[d]], recv_y.at[d])

        @pl.when(jnp.logical_not(first))
        def _():
            forward(ring[d])

    @pl.when(jnp.logical_not(first))
    def _():
        prepare()

    def group_rows(g):
        for y in range(RING):
            unpack(RING * g + y)
        block = win[8 * g : 8 * g + 8, 0:32, :].reshape(256, 128)
        return jnp.concatenate([block, tails[8 * g : 8 * g + 8].reshape(256, 128)], axis=1)

    unpack(1)

    @pl.when(first)
    def _():
        hear_z()

        @pl.when(core == 1)
        def _():
            pl.semaphore_wait(ready, 1)

        for d in (0,) + NEAR_FIRST:
            send_up(ring[d], here)
            send_down(ring[d])

    remote(mine, trans.at[pl.ds((1 - core) * half, half)], pair_send, pair_recv, sibling).wait_recv()
    lax.fori_loop(8 - core * 8, 16 - core * 8, pack_tails, 0)

    received(win.at[16:24], recv_z.at[1])
    unpack(2)
    spheres = 32 * groups
    shift = spheres + 32 - 32 * gx
    nothing = jnp.zeros((8, 128), F32)

    def picked_rows(q):
        mains, ends = [], []
        for i in range(0, 16, 2):
            pair = []
            for u in range(2):
                s = source[quarter * pairs + 16 * q + i + u]
                pair.append(window[jnp.minimum(lax.rem(s + shift, spheres), 95)])
            mains += [
                jnp.concatenate([pair[0][:, 0:128], nothing], axis=1),
                jnp.concatenate([nothing, pair[1][:, 0:128]], axis=1),
            ]
            for u in range(2):
                end = jnp.where(lane // 32 == (i + u) % 4, pair[u][:, 128:256], 0.0)
                ends.append(jnp.concatenate([end, nothing] if i % 8 < 4 else [nothing, end], axis=1))
        return jnp.concatenate(mains, axis=0).astype(BF16), jnp.concatenate(ends, axis=0).astype(BF16)

    received(win.at[0:4], recv_z.at[0])
    unpack(0, range(4))
    received(win.at[4:8], recv_z.at[2])
    unpack(0, range(4, 8))
    lane_of = lax.broadcasted_iota(jnp.int32, (80, 128), 1)
    sums_at = None
    for c in range(4):
        contrib = []
        for v in range(2):
            q = 2 * c + v
            mains, ends = picked_rows(q)
            blocks = [
                jnp.concatenate([trans[16 * q + 2 * j, :, 0:128], trans[16 * q + 2 * j + 1, :, 0:128]], axis=1)
                for j in range(8)
            ]
            main = lax.dot_general(
                jnp.concatenate(blocks, axis=0),
                mains,
                NT,
                preferred_element_type=F32,
            )
            end = lax.dot_general(
                ends_of[2 * q : 2 * q + 2].reshape(160, 256),
                ends,
                NT,
                preferred_element_type=F32,
            )
            total = jnp.where(lane_of < 64, end[0:80], end[80:160])
            half_sum = main[0:80]
            for j in range(1, 8):
                half_sum = jnp.where(lane_of // 16 == j, main[80 * j : 80 * j + 80], half_sum)
            contrib.append((total + half_sum).astype(BF16))
        part = lax.dot_general(
            place[:, 256 * c : 256 * c + 256], jnp.concatenate(contrib, axis=1), NT, preferred_element_type=F32
        )
        sums_at = part if sums_at is None else sums_at + part
    near = sums_at.astype(BF16)

    for j in range(16):
        for u in range(2):
            both = jnp.dot(near[16 * j : 16 * j + 16], wide[2 * j + u], preferred_element_type=F32)
            scat[2 * j + u] = both[8 * u : 8 * u + 8]

    for y in range(RING):
        h, r = 16 * (y // 4), 2 * (y % 4)
        rows = [scat[h : h + 16, r + u, 0:128] for u in range(2)]
        ends = [scat[h + 8 * (j % 2) : h + 8 * (j % 2) + 8, r + j // 2, 128:256] for j in range(4)]
        tail = ends[3]
        for v in range(3):
            tail = jnp.where(lane // 32 == v, ends[v], tail)
        parts[y] = jnp.concatenate(rows + [tail], axis=0).astype(BF16)
    for d in FAR_FIRST:
        remote(parts.at[ring[d]], sums.at[here], send_out, recv_out, at(gx, ring[d], core)).start()
    sums[here] = parts[here]
    remote(parts.at[0:7], sums.at[0:7], send_out, recv_out, sibling).wait_recv()
    total = sums[...].astype(F32).sum(axis=0)
    whole = jnp.concatenate([total[0:32], tail_rows(total[32:40])], axis=1)
    out[...] = (coeffs[...].astype(F32) - whole.reshape(2, 16, 160)).astype(BF16)
    remote(win.at[0:23], win.at[0:23], send_one, recv_y.at[0], sibling).wait_send()

    remote(parts.at[0:7], sums.at[0:7], send_out, recv_out, sibling).wait_send()
    send_pair.wait_send()


def solution(mesh):
    groups = mesh.shape["gx"]

    def step(coeffs, translations, tmatrix, pair_target, pair_source, pair_count):
        half = translations.shape[0]
        hbm = pl.BlockSpec(memory_space=pltpu.HBM)
        return pl.pallas_call(
            functools.partial(kernel, groups),
            out_shape=pltpu.VMEM(coeffs.shape, BF16),
            in_specs=[pl.BlockSpec(memory_space=pltpu.SMEM)] + [hbm] * 5,
            out_specs=pl.BlockSpec(memory_space=pltpu.VMEM),
            scratch_shapes=[
                pltpu.SMEM(pair_target.shape, jnp.int32),
                pltpu.SMEM(pair_source.shape, jnp.int32),
                pltpu.VMEM(coeffs.shape, BF16),
                pltpu.VMEM((2 * half, 80, 160), BF16),
                pltpu.VMEM((32, 80, 160), BF16),
                pltpu.VMEM((24, 40, 128), BF16),
                pltpu.VMEM((96, 8, 256), F32),
                pltpu.VMEM((16, 80, 256), BF16),
                pltpu.VMEM((256, 1024), BF16),
                pltpu.VMEM((32, 80, 256), BF16),
                pltpu.VMEM((32, 8, 256), F32),
                pltpu.VMEM((8, 40, 128), BF16),
                pltpu.VMEM((8, 40, 128), BF16),
                pltpu.SemaphoreType.DMA((5,)),
                pltpu.SemaphoreType.REGULAR,
                pltpu.SemaphoreType.DMA,
                pltpu.SemaphoreType.DMA((8,)),
                pltpu.SemaphoreType.DMA((3,)),
                pltpu.SemaphoreType.DMA,
                pltpu.SemaphoreType.DMA,
                pltpu.SemaphoreType.DMA,
                pltpu.SemaphoreType.DMA,
            ],
            compiler_params=pltpu.CompilerParams(
                collective_id=0, has_side_effects=True, vmem_limit_bytes=67_000_000
            ),
        )(pair_count, pair_target, pair_source, coeffs, translations, tmatrix)

    placed = (
        P("gz", ("gx", "gy"), None),
        P(("gx", "gz"), "gy", None),
        P("gx", "gy", None),
        P("gx"),
        P("gx"),
        P("gx"),
    )
    return jax.shard_map(
        step, mesh=mesh, in_specs=placed, out_specs=P("gz", ("gx", "gy"), None), check_vma=False
    )
```

```python
import functools

import jax
import jax.numpy as jnp
from jax import lax
from jax.experimental import pallas as pl
from jax.experimental.pallas import tpu as pltpu
from jax.sharding import PartitionSpec as P

MESH = pl.DeviceIdType.MESH
F32 = jnp.float32
BF16 = jnp.bfloat16
NT = (((1,), (1,)), ((), ()))
RING = 8
NEAR_FIRST = (1, 7, 2, 6, 3, 5, 4)
FAR_FIRST = (4, 3, 5, 2, 6, 1, 7)


def packed_rows(rows):
    tails = [rows[8 * j : 8 * j + 8, 128:160] for j in range(4)]
    tail = jnp.concatenate(tails, axis=1)
    return jnp.concatenate([rows[:, :128], tail], axis=0)


def tail_rows(tail):
    return jnp.concatenate([tail[:, 32 * j : 32 * j + 32] for j in range(4)], axis=0)


def kernel(
    groups, count, target_hbm, source_hbm, coeffs_hbm, trans_hbm, tmat_hbm, out,
    target, source, coeffs, trans, tmat, win, window, ends_of, place, wide, scat, parts, sums,
    local_sem, ready, recv_y, recv_z, pair_recv, recv_out,
):
    send_one, pair_send, send_out = local_sem.at[0], local_sem.at[1], local_sem.at[2]
    load_c = pltpu.make_async_copy(coeffs_hbm, coeffs, local_sem.at[0])
    load_c.start()

    gx, gy, gz = lax.axis_index("gx"), lax.axis_index("gy"), lax.axis_index("gz")
    quarter, core = gz // 2, gz % 2
    here = gy * 4 + quarter
    half = trans_hbm.shape[0]
    pairs = 2 * half
    above, below = (gx + 1) % groups, (gx + groups - 1) % groups
    first, last = gx % RING == 0, gx % RING == RING - 1
    lane = lax.broadcasted_iota(jnp.int32, (8, 128), 1)
    sub = lax.broadcasted_iota(jnp.int32, (8, 128), 0)
    sibling = {"gx": gx, "gy": gy, "gz": quarter * 2 + 1 - core}
    ring = [(here + d) % RING for d in range(RING)]

    def at(group, y, c):
        return {"gx": group, "gy": y // 4, "gz": (y % 4) * 2 + c}

    barrier = pltpu.get_barrier_semaphore()

    def greet(peer):
        pl.semaphore_signal(barrier, inc=1, device_id=peer, device_id_type=MESH)

    @pl.when(gx % RING == RING - 2)
    def _():
        greet(at(above, here, 1))

    @pl.when(gx % RING != RING - 2)
    def _():
        greet(at(above, here, 0))

    greet(at(below, here, 0))
    greet(sibling)
    for d in FAR_FIRST:
        greet(at(gx, ring[d], 1))

    @pl.when(first)
    def _():
        for d in FAR_FIRST:
            greet(at(below, ring[d], 0))

    load_p = [
        pltpu.make_async_copy(target_hbm, target, local_sem.at[3]),
        pltpu.make_async_copy(source_hbm, source, local_sem.at[4]),
    ]
    load_t = pltpu.make_async_copy(trans_hbm, trans.at[pl.ds(core * half, half)], local_sem.at[1])
    load_m = pltpu.make_async_copy(tmat_hbm, tmat, local_sem.at[2])
    for load in load_p:
        load.start()
    load_t.start()
    load_m.start()

    def tell_sibling():
        pl.semaphore_signal(ready, inc=1, device_id=sibling, device_id_type=MESH)

    def hear_z():
        @pl.when(core == 0)
        def _():
            pl.semaphore_wait(barrier, jnp.where(last, 1 + 2 * RING, 5))
            tell_sibling()

    @pl.when(jnp.logical_not(first))
    def _():
        hear_z()

    load_c.wait()
    own = coeffs[...].astype(F32).reshape(32, 160)
    win[RING + here] = packed_rows(own).astype(BF16)

    def remote(src, dst, s, r, peer):
        return pltpu.make_async_remote_copy(
            src_ref=src, dst_ref=dst, send_sem=s, recv_sem=r, device_id=peer, device_id_type=MESH
        )

    def send_up(y, to):
        remote(win.at[RING + y], win.at[y], send_one, recv_z.at[2 * (y // 4)], at(above, to, core)).start()

    def send_down(y):
        remote(win.at[RING + y], win.at[2 * RING + y], send_one, recv_z.at[1], at(below, here, core)).start()

    def forward(y):
        @pl.when(jnp.logical_not(last))
        def _():
            send_up(y, here)

        send_down(y)

    @pl.when(jnp.logical_not(first))
    def _():
        @pl.when(core == 1)
        def _():
            pl.semaphore_wait(ready, 1)

        @pl.when(last)
        def _():
            for d in FAR_FIRST + (0,):
                send_up(here, ring[d])

        @pl.when(jnp.logical_not(last))
        def _():
            forward(here)

    @pl.when(core == 1)
    def _():
        pl.semaphore_wait(barrier, jnp.where(last, 1 + 2 * RING, 2 * RING - 1))
        tell_sibling()

    @pl.when(core == 0)
    def _():
        pl.semaphore_wait(ready, 1)

    for d in FAR_FIRST:
        remote(
            win.at[RING + here], win.at[RING + here], send_one, recv_y.at[RING - 1 - d], at(gx, ring[d], core)
        ).start()

    @pl.when(last)
    def _():
        send_down(here)

    load_t.wait()
    mine = trans.at[pl.ds(core * half, half)]
    send_pair = remote(mine, mine, pair_send, pair_recv, sibling)
    send_pair.start()

    def unpack(group, blocks=range(RING)):
        for y in blocks:
            block = win[RING * group + y].astype(F32)
            base, r = 32 * group + 16 * (y // 4), 2 * (y % 4)
            packed = block[32:40]
            turned = [packed] + [pltpu.roll(packed, 32 * j, 1) for j in range(1, 4)]
            for j in range(4):
                tail = turned[(3 - j) % 4]
                for v in range(3):
                    tail = jnp.where(lane // 32 == v, turned[(v - j) % 4], tail)
                rows = pl.ds(base + 8 * (j % 2), 8)
                window[rows, r + j // 2, 0:128] = block[8 * j : 8 * j + 8]
                window[rows, r + j // 2, 128:256] = tail

    def received(blocks, sem):
        remote(blocks, blocks, send_one, sem, sibling).wait_recv()

    def pack_tails(m, carry):
        ends = [trans[8 * m + i, :, 128:160] for i in range(8)]
        ends_of[m] = jnp.concatenate(ends, axis=1)
        return carry

    def repeat_ends(m, carry):
        for u in range(4):
            block = tmat[4 * m + u]
            wide[4 * m + u] = jnp.concatenate([block[:, 0:128]] + [block[:, 128:160]] * 4, axis=1)
        return carry

    def build_place(q, carry):
        v = jnp.full((8, 128), -1, jnp.int32)
        for i in range(16):
            slot = quarter * pairs + q * 16 + i
            t = jnp.where(slot < count[0], target[slot], -1)
            v = jnp.where((lane // 8 == i) & (lane % 8 == sub), t, v)
        for s in range(16):
            hot = [jnp.where(v == 2 * s + u, 1.0, 0.0) for u in range(2)]
            place[16 * s : 16 * s + 16, pl.ds(pl.multiple_of(128 * q, 128), 128)] = jnp.concatenate(hot, axis=0).astype(BF16)
        return carry

    def prepare():
        for load in load_p:
            load.wait()
        lax.fori_loop(core * 8, core * 8 + 8, pack_tails, 0)
        load_m.wait()
        lax.fori_loop(0, 8, repeat_ends, 0)
        lax.fori_loop(0, pairs // 16, build_place, 0)

    @pl.when(first)
    def _():
        prepare()

    for d in NEAR_FIRST:
        received(win.at[RING + ring[d]], recv_y.at[d - 1])

        @pl.when(jnp.logical_not(first))
        def _():
            forward(ring[d])

    @pl.when(jnp.logical_not(first))
    def _():
        prepare()

    def group_rows(g):
        for y in range(RING):
            unpack(RING * g + y)
        block = win[8 * g : 8 * g + 8, 0:32, :].reshape(256, 128)
        return jnp.concatenate([block, tails[8 * g : 8 * g + 8].reshape(256, 128)], axis=1)

    unpack(1)

    @pl.when(first)
    def _():
        hear_z()

        @pl.when(core == 1)
        def _():
            pl.semaphore_wait(ready, 1)

        for d in (0,) + NEAR_FIRST:
            send_up(ring[d], here)
            send_down(ring[d])

    remote(mine, trans.at[pl.ds((1 - core) * half, half)], pair_send, pair_recv, sibling).wait_recv()
    lax.fori_loop(8 - core * 8, 16 - core * 8, pack_tails, 0)

    received(win.at[16:24], recv_z.at[1])
    unpack(2)
    spheres = 32 * groups
    shift = spheres + 32 - 32 * gx
    nothing = jnp.zeros((8, 128), F32)

    def picked_rows(q):
        mains, ends = [], []
        for i in range(0, 16, 2):
            pair = []
            for u in range(2):
                s = source[quarter * pairs + 16 * q + i + u]
                pair.append(window[jnp.minimum(lax.rem(s + shift, spheres), 95)])
            mains += [
                jnp.concatenate([pair[0][:, 0:128], nothing], axis=1),
                jnp.concatenate([nothing, pair[1][:, 0:128]], axis=1),
            ]
            for u in range(2):
                end = jnp.where(lane // 32 == (i + u) % 4, pair[u][:, 128:256], 0.0)
                ends.append(jnp.concatenate([end, nothing] if i % 8 < 4 else [nothing, end], axis=1))
        return jnp.concatenate(mains, axis=0).astype(BF16), jnp.concatenate(ends, axis=0).astype(BF16)

    received(win.at[0:4], recv_z.at[0])
    unpack(0, range(4))
    received(win.at[4:8], recv_z.at[2])
    unpack(0, range(4, 8))
    lane_of = lax.broadcasted_iota(jnp.int32, (80, 128), 1)
    sums_at = None
    for c in range(4):
        contrib = []
        for v in range(2):
            q = 2 * c + v
            mains, ends = picked_rows(q)
            blocks = [
                jnp.concatenate([trans[16 * q + 2 * j, :, 0:128], trans[16 * q + 2 * j + 1, :, 0:128]], axis=1)
                for j in range(8)
            ]
            main = lax.dot_general(
                jnp.concatenate(blocks, axis=0),
                mains,
                NT,
                preferred_element_type=F32,
            )
            end = lax.dot_general(
                ends_of[2 * q : 2 * q + 2].reshape(160, 256),
                ends,
                NT,
                preferred_element_type=F32,
            )
            total = jnp.where(lane_of < 64, end[0:80], end[80:160])
            half_sum = main[0:80]
            for j in range(1, 8):
                half_sum = jnp.where(lane_of // 16 == j, main[80 * j : 80 * j + 80], half_sum)
            contrib.append((total + half_sum).astype(BF16))
        part = lax.dot_general(
            place[:, 256 * c : 256 * c + 256], jnp.concatenate(contrib, axis=1), NT, preferred_element_type=F32
        )
        sums_at = part if sums_at is None else sums_at + part
    near = sums_at.astype(BF16)

    for j in range(16):
        for u in range(2):
            both = jnp.dot(near[16 * j : 16 * j + 16], wide[2 * j + u], preferred_element_type=F32)
            scat[2 * j + u] = both[8 * u : 8 * u + 8]

    for y in range(RING):
        h, r = 16 * (y // 4), 2 * (y % 4)
        rows = [scat[h : h + 16, r + u, 0:128] for u in range(2)]
        ends = [scat[h + 8 * (j % 2) : h + 8 * (j % 2) + 8, r + j // 2, 128:256] for j in range(4)]
        tail = ends[3]
        for v in range(3):
            tail = jnp.where(lane // 32 == v, ends[v], tail)
        parts[y] = jnp.concatenate(rows + [tail], axis=0).astype(BF16)
    for d in FAR_FIRST:
        remote(parts.at[ring[d]], sums.at[here], send_out, recv_out, at(gx, ring[d], core)).start()
    sums[here] = parts[here]
    remote(parts.at[0:7], sums.at[0:7], send_out, recv_out, sibling).wait_recv()
    total = sums[...].astype(F32).sum(axis=0)
    whole = jnp.concatenate([total[0:32], tail_rows(total[32:40])], axis=1)
    out[...] = (coeffs[...].astype(F32) - whole.reshape(2, 16, 160)).astype(BF16)
    remote(win.at[0:23], win.at[0:23], send_one, recv_y.at[0], sibling).wait_send()

    remote(parts.at[0:7], sums.at[0:7], send_out, recv_out, sibling).wait_send()
    send_pair.wait_send()


def solution(mesh):
    groups = mesh.shape["gx"]

    def step(coeffs, translations, tmatrix, pair_target, pair_source, pair_count):
        half = translations.shape[0]
        hbm = pl.BlockSpec(memory_space=pltpu.HBM)
        return pl.pallas_call(
            functools.partial(kernel, groups),
            out_shape=pltpu.VMEM(coeffs.shape, BF16),
            in_specs=[pl.BlockSpec(memory_space=pltpu.SMEM)] + [hbm] * 5,
            out_specs=pl.BlockSpec(memory_space=pltpu.VMEM),
            scratch_shapes=[
                pltpu.SMEM(pair_target.shape, jnp.int32),
                pltpu.SMEM(pair_source.shape, jnp.int32),
                pltpu.VMEM(coeffs.shape, BF16),
                pltpu.VMEM((2 * half, 80, 160), BF16),
                pltpu.VMEM((32, 80, 160), BF16),
                pltpu.VMEM((24, 40, 128), BF16),
                pltpu.VMEM((96, 8, 256), F32),
                pltpu.VMEM((16, 80, 256), BF16),
                pltpu.VMEM((256, 1024), BF16),
                pltpu.VMEM((32, 80, 256), BF16),
                pltpu.VMEM((32, 8, 256), F32),
                pltpu.VMEM((8, 40, 128), BF16),
                pltpu.VMEM((8, 40, 128), BF16),
                pltpu.SemaphoreType.DMA((5,)),
                pltpu.SemaphoreType.REGULAR,
                pltpu.SemaphoreType.DMA((RING - 1,)),
                pltpu.SemaphoreType.DMA((3,)),
                pltpu.SemaphoreType.DMA,
                pltpu.SemaphoreType.DMA,
            ],
            compiler_params=pltpu.CompilerParams(
                collective_id=0, has_side_effects=True, vmem_limit_bytes=67_000_000
            ),
        )(pair_count, pair_target, pair_source, coeffs, translations, tmatrix)

    placed = (
        P("gz", ("gx", "gy"), None),
        P(("gx", "gz"), "gy", None),
        P("gx", "gy", None),
        P("gx"),
        P("gx"),
        P("gx"),
    )
    return jax.shard_map(
        step, mesh=mesh, in_specs=placed, out_specs=P("gz", ("gx", "gy"), None), check_vma=False
    )
```

```python
import functools

import jax
import jax.numpy as jnp
from jax import lax
from jax.experimental import pallas as pl
from jax.experimental.pallas import tpu as pltpu
from jax.sharding import PartitionSpec as P

MESH = pl.DeviceIdType.MESH
F32 = jnp.float32
BF16 = jnp.bfloat16
NT = (((1,), (1,)), ((), ()))
RING = 8
NEAR_FIRST = (1, 7, 2, 6, 3, 5, 4)
FAR_FIRST = (4, 3, 5, 2, 6, 1, 7)


def packed_rows(rows):
    tails = [rows[8 * j : 8 * j + 8, 128:160] for j in range(4)]
    tail = jnp.concatenate(tails, axis=1)
    return jnp.concatenate([rows[:, :128], tail], axis=0)


def tail_rows(tail):
    return jnp.concatenate([tail[:, 32 * j : 32 * j + 32] for j in range(4)], axis=0)


def kernel(
    groups, count, target_hbm, source_hbm, coeffs_hbm, trans_hbm, tmat_hbm, out,
    target, source, coeffs, trans, tmat, win, window, ends_of, place, wide, scat, parts, sums,
    local_sem, ready, recv_y, recv_z, pair_recv, recv_out,
):
    send_one, pair_send, send_out = local_sem.at[0], local_sem.at[1], local_sem.at[2]
    load_c = pltpu.make_async_copy(coeffs_hbm, coeffs, local_sem.at[0])
    load_c.start()

    gx, gy, gz = lax.axis_index("gx"), lax.axis_index("gy"), lax.axis_index("gz")
    quarter, core = gz // 2, gz % 2
    here = gy * 4 + quarter
    half = trans_hbm.shape[0]
    pairs = 2 * half
    above, below = (gx + 1) % groups, (gx + groups - 1) % groups
    first, last = gx % RING == 0, gx % RING == RING - 1
    lane = lax.broadcasted_iota(jnp.int32, (8, 128), 1)
    sub = lax.broadcasted_iota(jnp.int32, (8, 128), 0)
    sibling = {"gx": gx, "gy": gy, "gz": quarter * 2 + 1 - core}
    ring = [(here + d) % RING for d in range(RING)]

    def at(group, y, c):
        return {"gx": group, "gy": y // 4, "gz": (y % 4) * 2 + c}

    barrier = pltpu.get_barrier_semaphore()

    def greet(peer):
        pl.semaphore_signal(barrier, inc=1, device_id=peer, device_id_type=MESH)

    @pl.when(gx % RING == RING - 2)
    def _():
        greet(at(above, here, 1))

    @pl.when(gx % RING != RING - 2)
    def _():
        greet(at(above, here, 0))

    greet(at(below, here, 0))
    greet(sibling)
    for d in FAR_FIRST:
        greet(at(gx, ring[d], 1))

    @pl.when(first)
    def _():
        for d in FAR_FIRST:
            greet(at(below, ring[d], 0))

    load_p = [
        pltpu.make_async_copy(target_hbm, target, local_sem.at[3]),
        pltpu.make_async_copy(source_hbm, source, local_sem.at[4]),
    ]
    load_t = pltpu.make_async_copy(trans_hbm, trans.at[pl.ds(core * half, half)], local_sem.at[1])
    load_m = pltpu.make_async_copy(tmat_hbm, tmat, local_sem.at[2])
    for load in load_p:
        load.start()
    load_t.start()
    load_m.start()

    def tell_sibling():
        pl.semaphore_signal(ready, inc=1, device_id=sibling, device_id_type=MESH)

    def hear_z():
        @pl.when(core == 0)
        def _():
            pl.semaphore_wait(barrier, jnp.where(last, 1 + 2 * RING, 5))
            tell_sibling()

    @pl.when(jnp.logical_not(first))
    def _():
        hear_z()

    load_c.wait()
    own = coeffs[...].astype(F32).reshape(32, 160)
    win[RING + here] = packed_rows(own).astype(BF16)

    def remote(src, dst, s, r, peer):
        return pltpu.make_async_remote_copy(
            src_ref=src, dst_ref=dst, send_sem=s, recv_sem=r, device_id=peer, device_id_type=MESH
        )

    def send_up(y, to):
        remote(win.at[RING + y], win.at[y], send_one, recv_z.at[y // 2], at(above, to, core)).start()

    def send_down(y):
        remote(win.at[RING + y], win.at[2 * RING + y], send_one, recv_z.at[4], at(below, here, core)).start()

    def forward(y):
        @pl.when(jnp.logical_not(last))
        def _():
            send_up(y, here)

        send_down(y)

    @pl.when(jnp.logical_not(first))
    def _():
        @pl.when(core == 1)
        def _():
            pl.semaphore_wait(ready, 1)

        @pl.when(last)
        def _():
            for d in FAR_FIRST + (0,):
                send_up(here, ring[d])

        @pl.when(jnp.logical_not(last))
        def _():
            forward(here)

    @pl.when(core == 1)
    def _():
        pl.semaphore_wait(barrier, jnp.where(last, 1 + 2 * RING, 2 * RING - 1))
        tell_sibling()

    @pl.when(core == 0)
    def _():
        pl.semaphore_wait(ready, 1)

    for d in FAR_FIRST:
        remote(
            win.at[RING + here], win.at[RING + here], send_one, recv_y.at[RING - 1 - d], at(gx, ring[d], core)
        ).start()

    @pl.when(last)
    def _():
        send_down(here)

    load_t.wait()
    mine = trans.at[pl.ds(core * half, half)]
    send_pair = remote(mine, mine, pair_send, pair_recv, sibling)
    send_pair.start()

    def unpack(group, blocks=range(RING)):
        for y in blocks:
            block = win[RING * group + y].astype(F32)
            base, r = 32 * group + 16 * (y // 4), 2 * (y % 4)
            packed = block[32:40]
            turned = [packed] + [pltpu.roll(packed, 32 * j, 1) for j in range(1, 4)]
            for j in range(4):
                tail = turned[(3 - j) % 4]
                for v in range(3):
                    tail = jnp.where(lane // 32 == v, turned[(v - j) % 4], tail)
                rows = pl.ds(base + 8 * (j % 2), 8)
                window[rows, r + j // 2, 0:128] = block[8 * j : 8 * j + 8]
                window[rows, r + j // 2, 128:256] = tail

    def received(blocks, sem):
        remote(blocks, blocks, send_one, sem, sibling).wait_recv()

    def pack_tails(m, carry):
        ends = [trans[8 * m + i, :, 128:160] for i in range(8)]
        ends_of[m] = jnp.concatenate(ends, axis=1)
        return carry

    def repeat_ends(m, carry):
        for u in range(4):
            block = tmat[4 * m + u]
            wide[4 * m + u] = jnp.concatenate([block[:, 0:128]] + [block[:, 128:160]] * 4, axis=1)
        return carry

    def build_place(q, carry):
        v = jnp.full((8, 128), -1, jnp.int32)
        for i in range(16):
            slot = quarter * pairs + q * 16 + i
            t = jnp.where(slot < count[0], target[slot], -1)
            v = jnp.where((lane // 8 == i) & (lane % 8 == sub), t, v)
        for s in range(16):
            hot = [jnp.where(v == 2 * s + u, 1.0, 0.0) for u in range(2)]
            place[16 * s : 16 * s + 16, pl.ds(pl.multiple_of(128 * q, 128), 128)] = jnp.concatenate(hot, axis=0).astype(BF16)
        return carry

    def prepare():
        for load in load_p:
            load.wait()
        lax.fori_loop(core * 8, core * 8 + 8, pack_tails, 0)
        load_m.wait()
        lax.fori_loop(0, 8, repeat_ends, 0)
        lax.fori_loop(0, pairs // 16, build_place, 0)

    @pl.when(first)
    def _():
        prepare()

    for d in NEAR_FIRST:
        received(win.at[RING + ring[d]], recv_y.at[d - 1])

        @pl.when(jnp.logical_not(first))
        def _():
            forward(ring[d])

    @pl.when(jnp.logical_not(first))
    def _():
        prepare()

    def group_rows(g):
        for y in range(RING):
            unpack(RING * g + y)
        block = win[8 * g : 8 * g + 8, 0:32, :].reshape(256, 128)
        return jnp.concatenate([block, tails[8 * g : 8 * g + 8].reshape(256, 128)], axis=1)

    unpack(1)

    @pl.when(first)
    def _():
        hear_z()

        @pl.when(core == 1)
        def _():
            pl.semaphore_wait(ready, 1)

        for d in (0,) + NEAR_FIRST:
            send_up(ring[d], here)
            send_down(ring[d])

    remote(mine, trans.at[pl.ds((1 - core) * half, half)], pair_send, pair_recv, sibling).wait_recv()
    lax.fori_loop(8 - core * 8, 16 - core * 8, pack_tails, 0)

    received(win.at[16:24], recv_z.at[4])
    unpack(2)
    spheres = 32 * groups
    shift = spheres + 32 - 32 * gx
    nothing = jnp.zeros((8, 128), F32)

    def picked_rows(q):
        mains, ends = [], []
        for i in range(0, 16, 2):
            pair = []
            for u in range(2):
                s = source[quarter * pairs + 16 * q + i + u]
                pair.append(window[jnp.minimum(lax.rem(s + shift, spheres), 95)])
            mains += [
                jnp.concatenate([pair[0][:, 0:128], nothing], axis=1),
                jnp.concatenate([nothing, pair[1][:, 0:128]], axis=1),
            ]
            for u in range(2):
                end = jnp.where(lane // 32 == (i + u) % 4, pair[u][:, 128:256], 0.0)
                ends.append(jnp.concatenate([end, nothing] if i % 8 < 4 else [nothing, end], axis=1))
        return jnp.concatenate(mains, axis=0).astype(BF16), jnp.concatenate(ends, axis=0).astype(BF16)

    for v in (0, 1, 3, 2):
        received(win.at[2 * v : 2 * v + 2], recv_z.at[v])
        unpack(0, range(2 * v, 2 * v + 2))
    lane_of = lax.broadcasted_iota(jnp.int32, (80, 128), 1)
    sums_at = None
    for c in range(4):
        contrib = []
        for v in range(2):
            q = 2 * c + v
            mains, ends = picked_rows(q)
            blocks = [
                jnp.concatenate([trans[16 * q + 2 * j, :, 0:128], trans[16 * q + 2 * j + 1, :, 0:128]], axis=1)
                for j in range(8)
            ]
            main = lax.dot_general(
                jnp.concatenate(blocks, axis=0),
                mains,
                NT,
                preferred_element_type=F32,
            )
            end = lax.dot_general(
                ends_of[2 * q : 2 * q + 2].reshape(160, 256),
                ends,
                NT,
                preferred_element_type=F32,
            )
            total = jnp.where(lane_of < 64, end[0:80], end[80:160])
            half_sum = main[0:80]
            for j in range(1, 8):
                half_sum = jnp.where(lane_of // 16 == j, main[80 * j : 80 * j + 80], half_sum)
            contrib.append((total + half_sum).astype(BF16))
        part = lax.dot_general(
            place[:, 256 * c : 256 * c + 256], jnp.concatenate(contrib, axis=1), NT, preferred_element_type=F32
        )
        sums_at = part if sums_at is None else sums_at + part
    near = sums_at.astype(BF16)

    for j in range(16):
        for u in range(2):
            both = jnp.dot(near[16 * j : 16 * j + 16], wide[2 * j + u], preferred_element_type=F32)
            scat[2 * j + u] = both[8 * u : 8 * u + 8]

    for y in range(RING):
        h, r = 16 * (y // 4), 2 * (y % 4)
        rows = [scat[h : h + 16, r + u, 0:128] for u in range(2)]
        ends = [scat[h + 8 * (j % 2) : h + 8 * (j % 2) + 8, r + j // 2, 128:256] for j in range(4)]
        tail = ends[3]
        for v in range(3):
            tail = jnp.where(lane // 32 == v, ends[v], tail)
        parts[y] = jnp.concatenate(rows + [tail], axis=0).astype(BF16)
    for d in FAR_FIRST:
        remote(parts.at[ring[d]], sums.at[here], send_out, recv_out, at(gx, ring[d], core)).start()
    sums[here] = parts[here]
    remote(parts.at[0:7], sums.at[0:7], send_out, recv_out, sibling).wait_recv()
    total = sums[...].astype(F32).sum(axis=0)
    whole = jnp.concatenate([total[0:32], tail_rows(total[32:40])], axis=1)
    out[...] = (coeffs[...].astype(F32) - whole.reshape(2, 16, 160)).astype(BF16)
    remote(win.at[0:23], win.at[0:23], send_one, recv_y.at[0], sibling).wait_send()

    remote(parts.at[0:7], sums.at[0:7], send_out, recv_out, sibling).wait_send()
    send_pair.wait_send()


def solution(mesh):
    groups = mesh.shape["gx"]

    def step(coeffs, translations, tmatrix, pair_target, pair_source, pair_count):
        half = translations.shape[0]
        hbm = pl.BlockSpec(memory_space=pltpu.HBM)
        return pl.pallas_call(
            functools.partial(kernel, groups),
            out_shape=pltpu.VMEM(coeffs.shape, BF16),
            in_specs=[pl.BlockSpec(memory_space=pltpu.SMEM)] + [hbm] * 5,
            out_specs=pl.BlockSpec(memory_space=pltpu.VMEM),
            scratch_shapes=[
                pltpu.SMEM(pair_target.shape, jnp.int32),
                pltpu.SMEM(pair_source.shape, jnp.int32),
                pltpu.VMEM(coeffs.shape, BF16),
                pltpu.VMEM((2 * half, 80, 160), BF16),
                pltpu.VMEM((32, 80, 160), BF16),
                pltpu.VMEM((24, 40, 128), BF16),
                pltpu.VMEM((96, 8, 256), F32),
                pltpu.VMEM((16, 80, 256), BF16),
                pltpu.VMEM((256, 1024), BF16),
                pltpu.VMEM((32, 80, 256), BF16),
                pltpu.VMEM((32, 8, 256), F32),
                pltpu.VMEM((8, 40, 128), BF16),
                pltpu.VMEM((8, 40, 128), BF16),
                pltpu.SemaphoreType.DMA((5,)),
                pltpu.SemaphoreType.REGULAR,
                pltpu.SemaphoreType.DMA((RING - 1,)),
                pltpu.SemaphoreType.DMA((5,)),
                pltpu.SemaphoreType.DMA,
                pltpu.SemaphoreType.DMA,
            ],
            compiler_params=pltpu.CompilerParams(
                collective_id=0, has_side_effects=True, vmem_limit_bytes=67_000_000
            ),
        )(pair_count, pair_target, pair_source, coeffs, translations, tmatrix)

    placed = (
        P("gz", ("gx", "gy"), None),
        P(("gx", "gz"), "gy", None),
        P("gx", "gy", None),
        P("gx"),
        P("gx"),
        P("gx"),
    )
    return jax.shard_map(
        step, mesh=mesh, in_specs=placed, out_specs=P("gz", ("gx", "gy"), None), check_vma=False
    )
```
